16 devices in a mesh: rep: 1, r: 4 (over y, z), s: 4 (over x, core).
Axes of the slice: x: 2, y: 2, z: 2, core: 2. Of those that a mesh axis runs over, the one named last changes fastest.
Arguments:
- x: bfloat16 [16, 4096, 896], P(('rep', 'r', 's'))
- dy: bfloat16 [16, 4096, 896], P(('rep', 'r', 's'))
- w_gate: bfloat16 [2, 896, 2560], P(None, 's')
- w_up: bfloat16 [2, 896, 2560], P(None, 's')
- w_down: bfloat16 [2, 2560, 896], P(None, 's')
- m_w_gate: float32 [2, 896, 2560], P(None, 's')
- m_w_up: float32 [2, 896, 2560], P(None, 's')
- m_w_down: float32 [2, 2560, 896], P(None, 's')
- v_w_gate: float32 [2, 896, 2560], P(None, 's')
- v_w_up: float32 [2, 896, 2560], P(None, 's')
- v_w_down: float32 [2, 2560, 896], P(None, 's')
Outputs:
- output 1: bfloat16 [2, 896, 2560], P('rep', 's')
- output 2: bfloat16 [2, 896, 2560], P('rep', 's')
- output 3: bfloat16 [2, 2560, 896], P('rep', 's')
- output 4: float32 [2, 896, 2560], P('rep', 's')
- output 5: float32 [2, 896, 2560], P('rep', 's')
- output 6: float32 [2, 2560, 896], P('rep', 's')
- output 7: float32 [2, 896, 2560], P('rep', 's')
- output 8: float32 [2, 896, 2560], P('rep', 's')
- output 9: float32 [2, 2560, 896], P('rep', 's')
All inputs are finite; a program needn't handle non-finite values.
Results may differ from the reference program's by a relative error of at most 0.022.
Values are sent between devices in bfloat16 or wider.
A program may use at most 2 GiB of HBM per device.

```python
import jax
import jax.numpy as jnp
from jax import lax

SEQUENCES = 16
TOKENS = 4096
D = 896
FF = 2560
LAYERS = 2
NAMES = ("w_gate", "w_up", "w_down")
SHAPES = {"w_gate": (LAYERS, D, FF), "w_up": (LAYERS, D, FF), "w_down": (LAYERS, FF, D)}


def bump(key, n, height):
    away = (jnp.arange(n, dtype=jnp.int32) - jax.random.randint(key, (), 0, n, jnp.int32)) % n
    return jnp.where(away < n // 8, height, 1.0)


def together(key, own, strength):
    shared = jax.random.normal(key, own.shape[1:], jnp.float32)
    return (own + strength * shared) * lax.rsqrt(1 + strength * strength)


def setup_inputs(seed: int = 0, part: int = 0) -> dict:
    kx, kdy, ka, kb, kz, kf, kh, kl, *keys = jax.random.split(jax.random.key(seed), 8 + 3 * len(NAMES))
    kx, kdy, ka, kb = (jax.random.fold_in(k, part) for k in (kx, kdy, ka, kb))
    kw, km, kv = (keys[i::3] for i in range(3))
    shape = (SEQUENCES, TOKENS, D)
    much_x, much_dy = jax.random.uniform(kz, (2,), jnp.float32, 0.0, 1.0)
    loud = 2.0 ** jax.random.uniform(jax.random.fold_in(kz, 1), (), jnp.float32, -1.0, 2.0)
    layers = 2.0 ** jax.random.uniform(kl, (LAYERS, 1, 1), jnp.float32, -1.0, 1.0)
    x = together(ka, jax.random.normal(kx, shape, jnp.float32), much_x) * bump(kf, D, 4.0)
    dy = together(kb, jax.random.normal(kdy, shape, jnp.float32), much_dy)
    drawn = {"x": x.astype(jnp.bfloat16), "dy": (loud * dy * (SEQUENCES * TOKENS) ** -0.5).astype(jnp.bfloat16)}
    for key, name in zip(kw, NAMES, strict=True):
        w = jax.random.normal(key, SHAPES[name], jnp.float32) * SHAPES[name][1] ** -0.5
        drawn[name] = (w * {"w_gate": 1.0, "w_up": bump(kh, FF, 4.0), "w_down": layers}[name]).astype(jnp.bfloat16)
    for key, name in zip(km, NAMES, strict=True):
        drawn[f"m_{name}"] = 0.1 * jax.random.normal(key, SHAPES[name], jnp.float32)
    for key, name in zip(kv, NAMES, strict=True):
        drawn[f"v_{name}"] = jax.random.uniform(key, SHAPES[name], jnp.float32, 0.005, 0.015)
    return drawn


def matmul(a, w):
    return jnp.dot(a, w, preferred_element_type=jnp.float32).astype(jnp.bfloat16)


def normed(h):
    wide = h.astype(jnp.float32)
    scale = lax.rsqrt(jnp.mean(wide**2, -1, keepdims=True) + 1e-6)
    return (wide * scale).astype(jnp.bfloat16)


def layer(h, w):
    a = normed(h)
    gate = jnp.dot(a, w["w_gate"], preferred_element_type=jnp.float32)
    up = jnp.dot(a, w["w_up"], preferred_element_type=jnp.float32)
    return h + matmul((jax.nn.silu(gate) * up).astype(jnp.bfloat16), w["w_down"])


def adamw(w, m, v, g):
    m = 0.9 * m + 0.1 * g
    v = 0.95 * v + 0.05 * g * g
    step = m * lax.rsqrt(v + 1e-8) + 0.1 * w
    return (w - 0.02 * step).astype(jnp.bfloat16), m, v


def clipped(gradients, sum_of_squares, count):
    factor = jnp.minimum(1.0, 0.5 * lax.rsqrt(sum_of_squares / count + 1e-30))
    return [g * factor for g in gradients]


def stack(weights, h):
    return lax.scan(lambda h, w: (layer(h, w), None), h, weights)[0]


def reference(x, dy, w_gate, w_up, w_down, m_w_gate, m_w_up, m_w_down, v_w_gate, v_w_up, v_w_down):
    weights = dict(zip(NAMES, (w_gate, w_up, w_down), strict=True))

    def take(so_far, sequence):
        h, by_y = sequence
        _, back = jax.vjp(lambda w: stack(w, h), weights)
        return jax.tree.map(lambda total, term: total + term.astype(jnp.float32), so_far, back(by_y)[0]), None

    none_yet = {name: jnp.zeros(w.shape, jnp.float32) for name, w in weights.items()}
    by_weights, _ = lax.scan(take, none_yet, (x, dy))
    gradients = [by_weights[name].astype(jnp.bfloat16).astype(jnp.float32) for name in NAMES]
    gradients = clipped(gradients, sum(jnp.sum(g * g) for g in gradients), sum(g.size for g in gradients))
    new = [
        adamw(w.astype(jnp.float32), m, v, g)
        for w, m, v, g in zip((w_gate, w_up, w_down), (m_w_gate, m_w_up, m_w_down), (v_w_gate, v_w_up, v_w_down), gradients, strict=True)
    ]
    return tuple(one[which] for which in range(3) for one in new)
```

```python
import functools

import jax
import jax.numpy as jnp
from jax import lax
from jax.experimental import pallas as pl
from jax.experimental.pallas import tpu as pltpu
from jax.sharding import PartitionSpec as P

NAMES = ("w_gate", "w_up", "w_down")
F32, BF16 = jnp.float32, jnp.bfloat16
VMEM_LIMIT = 60 * 1024 * 1024


def dot(a, b, dims):
    return lax.dot_general(a, b, (dims, ((), ())), preferred_element_type=F32)


NN, NT, TN = ((1,), (0,)), ((1,), (1,)), ((0,), (0,))


def normed(h):
    wide = h.astype(F32)
    scale = lax.rsqrt(jnp.mean(wide * wide, -1, keepdims=True) + 1e-6)
    return (wide * scale).astype(BF16)


def call(body, name, grid, in_specs, out_specs, out_shape, scratch, flops, moved):
    return pl.pallas_call(
        body,
        grid=grid,
        in_specs=in_specs,
        out_specs=out_specs,
        out_shape=out_shape,
        scratch_shapes=scratch,
        name=name,
        compiler_params=pltpu.CompilerParams(dimension_semantics=("arbitrary",) * len(grid), vmem_limit_bytes=VMEM_LIMIT),
        cost_estimate=pl.CostEstimate(flops=flops, bytes_accessed=moved, transcendentals=0),
    )


def once(shape, index):
    return pl.BlockSpec(shape, index, pipeline_mode=pl.Buffered(1))


def shape(dims, dtype):
    return jax.ShapeDtypeStruct(dims, dtype)


def project_body(part, h_ref, wg_ref, wu_ref, gate_ref, up_ref, prod_ref):
    a = normed(h_ref[...])
    for i in range(wg_ref.shape[1] // part):
        cols = slice(i * part, (i + 1) * part)
        gate = dot(a, wg_ref[:, cols], NN)
        up = dot(a, wu_ref[:, cols], NN)
        gate_ref[:, cols] = gate
        up_ref[:, cols] = up
        prod_ref[:, cols] = (gate * jax.nn.sigmoid(gate) * up).astype(BF16)


def project(h, wg, wu, tile=256, part=640):
    n, d = h.shape
    ff = wg.shape[1]
    rows = lambda width: pl.BlockSpec((tile, width), lambda i: (i, 0))
    return call(
        functools.partial(project_body, part),
        "project",
        (n // tile,),
        [rows(d), once((d, ff), lambda i: (0, 0)), once((d, ff), lambda i: (0, 0))],
        [rows(ff)] * 3,
        [shape((n, ff), F32), shape((n, ff), F32), shape((n, ff), BF16)],
        [],
        4 * n * d * ff,
        n * ff * 10,
    )(h, wg, wu)


def down_body(h_ref, prod_ref, wd_ref, out_ref):
    out_ref[...] = h_ref[...] + dot(prod_ref[...], wd_ref[...], NN).astype(BF16)


def down(h, prod, wd, tile=512):
    n, d = h.shape
    ff = wd.shape[0]
    rows = lambda width: pl.BlockSpec((tile, width), lambda i: (i, 0))
    return call(
        down_body,
        "down",
        (n // tile,),
        [rows(d), rows(ff), once((ff, d), lambda i: (0, 0))],
        rows(d),
        shape((n, d), BF16),
        [],
        2 * n * d * ff,
        n * ff * 2,
    )(h, prod, wd)


def spread(place, acc, rows, send_ref, far_ref, near_ref):
    x, c = place[0], place[1]

    def block(bx, bc):
        return acc[pl.ds(pl.multiple_of((bx * 2 + bc) * rows, rows), rows), :].astype(BF16)

    send_ref[0] = block(1 - x, 1 - c)
    send_ref[1] = block(x, 1 - c)
    far_ref[...] = block(1 - x, c)
    near_ref[...] = block(x, c)


def spread_shapes(rows, cols):
    return [shape((2, rows, cols), BF16), shape((rows, cols), BF16), shape((rows, cols), BF16)]


def spread_specs(rows, cols):
    return [once((2, rows, cols), lambda *_: (0, 0, 0)), once((rows, cols), lambda *_: (0, 0)), once((rows, cols), lambda *_: (0, 0))]


PLACE = pl.BlockSpec(memory_space=pltpu.SMEM)


def last_body(part, place, h_ref, dy_ref, wg_ref, wu_ref, wd_ref, dgate_ref, dup_ref, dwd_ref, *rest):
    outs, (acc_g, acc_u, acc_d) = rest[:6], rest[6:]
    step = pl.program_id(0)

    @pl.when(step == 0)
    def _():
        acc_g[...] = jnp.zeros_like(acc_g)
        acc_u[...] = jnp.zeros_like(acc_u)
        acc_d[...] = jnp.zeros_like(acc_d)

    a = normed(h_ref[...])
    dy = dy_ref[...]
    a_t, dy_t = a.T, dy.T
    for i in range(wg_ref.shape[1] // part):
        cols = slice(i * part, (i + 1) * part)
        gate = dot(a, wg_ref[:, cols], NN)
        up = dot(a, wu_ref[:, cols], NN)
        dprod = dot(dy, wd_ref[cols, :], NT).astype(BF16).astype(F32)
        s = jax.nn.sigmoid(gate)
        silu = gate * s
        prod = (silu * up).astype(BF16)
        dup = (dprod * silu).astype(BF16)
        dgate = (dprod * up * (s + silu * (1 - s))).astype(BF16)
        dgate_ref[:, cols] = dgate
        dup_ref[:, cols] = dup
        acc_g[:, cols] += dot(a_t, dgate, NN)
        acc_u[:, cols] += dot(a_t, dup, NN)
        acc_d[:, cols] += dot(dy_t, prod, NN)

    @pl.when(step == pl.num_programs(0) - 1)
    def _():
        rows = acc_g.shape[0] // 4
        spread(place, acc_g, rows, *outs[:3])
        spread(place, acc_u, rows, *outs[3:])
        dwd_ref[...] = acc_d[...].T.astype(BF16)


def last(place, h, dy, wg, wu, wd, run, runs, tile=256, part=256):
    n, d = h.shape
    ff = wg.shape[1] // runs
    rows = lambda width: pl.BlockSpec((tile, width), lambda i: (i, 0))
    columns = lambda: once((d, ff), lambda i: (0, run))
    outs = call(
        functools.partial(last_body, part),
        f"last{run}",
        (n // tile,),
        [PLACE, rows(d), rows(d), columns(), columns(), once((ff, d), lambda i: (run, 0))],
        [rows(ff), rows(ff), once((ff, d), lambda i: (0, 0))] + spread_specs(d // 4, ff) * 2,
        [shape((n, ff), BF16)] * 2 + [shape((ff, d), BF16)] + spread_shapes(d // 4, ff) * 2,
        [pltpu.VMEM((d, ff), F32)] * 3,
        12 * n * d * ff,
        n * ff * 4,
    )(place, h, dy, wg, wu, wd)
    return outs[0], outs[1], outs[2], outs[3:6], outs[6:9]


def inward_body(runs, h_ref, by_ref, *rest):
    dgates, dups, (wg_ref, wu_ref, out_ref) = rest[:runs], rest[runs : 2 * runs], rest[2 * runs :]
    ff = dgates[0].shape[1]
    total = lambda parts, w: sum(dot(p[...], w[:, i * ff : (i + 1) * ff], NT) for i, p in enumerate(parts)).astype(BF16)
    da = (total(dgates, wg_ref) + total(dups, wu_ref)).astype(F32)
    wide = h_ref[...].astype(F32)
    scale = lax.rsqrt(jnp.mean(wide * wide, -1, keepdims=True) + 1e-6)
    along = jnp.mean(da * wide, -1, keepdims=True)
    dh = da * scale - wide * (scale * scale * scale * along)
    out_ref[...] = by_ref[...] + dh.astype(BF16)


def inward(h, by, dgates, dups, wg, wu, tile=512):
    n, d = h.shape
    ff = wg.shape[1]
    runs = len(dgates)
    rows = lambda width: pl.BlockSpec((tile, width), lambda i: (i, 0))
    return call(
        functools.partial(inward_body, runs),
        "inward",
        (n // tile,),
        [rows(d), rows(d)] + [rows(ff // runs)] * (2 * runs) + [once((d, ff), lambda i: (0, 0))] * 2,
        rows(d),
        shape((n, d), BF16),
        [],
        4 * n * d * ff,
        n * ff * 4,
    )(h, by, *dgates, *dups, wg, wu)


def outer_body(place, by_ref, prod_ref, send_ref, far_ref, near_ref, acc, turned):
    step = pl.program_id(0)

    @pl.when(step == 0)
    def _():
        acc[...] = jnp.zeros_like(acc)

    by_t = by_ref[...].T
    acc[...] += dot(by_t, prod_ref[...], NN)

    @pl.when(step == pl.num_programs(0) - 1)
    def _():
        turned[...] = acc[...].T.astype(BF16)
        spread(place, turned, turned.shape[0] // 4, send_ref, far_ref, near_ref)


def outer(place, by, prod, tile=512):
    n, d = by.shape
    ff = prod.shape[1]
    rows = lambda width: pl.BlockSpec((tile, width), lambda i: (i, 0))
    return call(
        outer_body,
        "outer",
        (n // tile,),
        [PLACE, rows(d), rows(ff)],
        spread_specs(ff // 4, d),
        spread_shapes(ff // 4, d),
        [pltpu.VMEM((d, ff), F32), pltpu.VMEM((ff, d), BF16)],
        2 * n * d * ff,
        n * ff * 2,
    )(place, by, prod)


def first_body(part, place, h_ref, by_ref, gate_ref, up_ref, wd_ref, *rest):
    outs, (acc_g, acc_u) = rest[:6], rest[6:]
    step = pl.program_id(0)

    @pl.when(step == 0)
    def _():
        acc_g[...] = jnp.zeros_like(acc_g)
        acc_u[...] = jnp.zeros_like(acc_u)

    a_t = normed(h_ref[...]).T
    by = by_ref[...]
    for i in range(wd_ref.shape[0] // part):
        cols = slice(i * part, (i + 1) * part)
        dprod = dot(by, wd_ref[cols, :], NT).astype(BF16).astype(F32)
        gate, up = gate_ref[:, cols], up_ref[:, cols]
        s = jax.nn.sigmoid(gate)
        silu = gate * s
        dup = (dprod * silu).astype(BF16)
        dgate = (dprod * up * (s + silu * (1 - s))).astype(BF16)
        acc_g[:, cols] += dot(a_t, dgate, NN)
        acc_u[:, cols] += dot(a_t, dup, NN)

    @pl.when(step == pl.num_programs(0) - 1)
    def _():
        rows = acc_g.shape[0] // 4
        spread(place, acc_g, rows, *outs[:3])
        spread(place, acc_u, rows, *outs[3:])


def first(place, h, by, gate, up, wd, start, width, tile=512, part=256):
    n, d = h.shape
    run = start // width
    rows = lambda: pl.BlockSpec((tile, d), lambda i: (i, 0))
    kept = lambda: pl.BlockSpec((tile, width), lambda i: (i, run))
    outs = call(
        functools.partial(first_body, part),
        f"first{run}",
        (n // tile,),
        [PLACE, rows(), rows(), kept(), kept(), once((width, d), lambda i: (run, 0))],
        spread_specs(d // 4, width) * 2,
        spread_shapes(d // 4, width) * 2,
        [pltpu.VMEM((d, width), F32)] * 2,
        6 * n * d * width,
        n * width * 8,
    )(place, h, by, gate, up, wd)
    return outs[:3], outs[3:]


def adamw(w, m, v, g):
    m = 0.9 * m + 0.1 * g
    v = 0.95 * v + 0.05 * g * g
    step = m * lax.rsqrt(v + 1e-8) + 0.1 * w
    return (w - 0.02 * step).astype(BF16), m, v


def added(*terms):
    return sum(t.astype(F32) for t in terms).astype(BF16)


def solution(mesh):
    ns, nr = mesh.shape["s"], mesh.shape["r"]
    by_core = [(i, i ^ 1) for i in range(ns)]
    by_x = [(i, i ^ 2) for i in range(ns)]
    by_y = [(i, i ^ 2) for i in range(nr)]
    by_z = [(i, i ^ 1) for i in range(nr)]

    def fetched(weights, number):
        return [lax.all_gather(w[number], "s", axis=0, tiled=True) for w in weights]

    def summed(terms):
        send, far, near = terms
        got = lax.ppermute(send, "s", by_core)
        far = added(far, got[0])
        near = added(near, got[1], lax.ppermute(far, "s", by_x))
        half = near.shape[1] // 256 * 128
        a, b = near[:, :half], near[:, half:]
        a, b = added(a, lax.ppermute(a, "r", by_y)), added(b, lax.ppermute(b, "r", by_z))
        a, b = added(a, lax.ppermute(a, "r", by_z)), added(b, lax.ppermute(b, "r", by_y))
        return jnp.concatenate([a, b], axis=1)

    def sorted_terms(place, term):
        rows = term.shape[0] // 4
        x, c = place[0], place[1]
        blocks = term.reshape(2, 2, rows, term.shape[1])
        pick = lambda i, j: lax.dynamic_slice(blocks, (i, j, 0, 0), (1, 1) + blocks.shape[2:]).reshape(blocks.shape[2:])
        return jnp.stack([pick(1 - x, 1 - c), pick(x, 1 - c)]), pick(1 - x, c), pick(x, c)

    def step(x, dy, *arrays):
        weights, m, v = (arrays[i : i + 3] for i in (0, 3, 6))
        me = lax.axis_index("s")
        place = jnp.stack([me // 2, me % 2]).astype(jnp.int32)
        h0, dy = x[0], dy[0]
        wg0, wu0, wd0 = fetched(weights, 0)
        gate, up, prod = project(h0, wg0, wu0)
        h1 = down(h0, prod, wd0)
        wg1, wu1, wd1 = fetched(weights, 1)
        runs = 2
        lasts = [last(place, h1, dy, wg1, wu1, wd1, run, runs) for run in range(runs)]
        sums1 = [[summed(one[3]), summed(one[4])] for one in lasts]
        d1 = summed(sorted_terms(place, jnp.concatenate([one[2] for one in lasts])))
        by = inward(h1, dy, [one[0] for one in lasts], [one[1] for one in lasts], wg1, wu1)
        d0 = summed(outer(place, by, prod))
        widths = [1280, 1280]
        firsts = [first(place, h0, by, gate, up, wd0, sum(widths[:i]), w) for i, w in enumerate(widths)]
        sums0 = [[summed(one[0]), summed(one[1])] for one in firsts]
        joined = lambda sums, i: jnp.concatenate([one[i] for one in sums], axis=1)
        gradients = [
            jnp.stack([joined(sums0, 0), joined(sums1, 0)]).astype(F32),
            jnp.stack([joined(sums0, 1), joined(sums1, 1)]).astype(F32),
            jnp.stack([d0, d1]).astype(F32),
        ]
        squares = lax.psum(sum(jnp.sum(g * g) for g in gradients), "s")
        count = ns * sum(g.size for g in gradients)
        factor = jnp.minimum(1.0, 0.5 * lax.rsqrt(squares / count + 1e-30))
        new = [adamw(w.astype(F32), m, v, g * factor) for w, m, v, g in zip(weights, m, v, gradients, strict=True)]
        return tuple(one[which] for which in range(3) for one in new)

    states, cut = P(("rep", "r", "s"), None, None), P(None, "s", None)
    return jax.shard_map(
        step,
        mesh=mesh,
        in_specs=(states, states) + (cut,) * 9,
        out_specs=(P("rep", "s", None),) * 9,
        check_vma=False,
    )
```

```python
import functools

import jax
import jax.numpy as jnp
from jax import lax
from jax.experimental import pallas as pl
from jax.experimental.pallas import tpu as pltpu
from jax.sharding import PartitionSpec as P

NAMES = ("w_gate", "w_up", "w_down")
F32, BF16 = jnp.float32, jnp.bfloat16
MESH = pl.DeviceIdType.MESH
VMEM_LIMIT = 60 * 1024 * 1024
SMALL = VMEM_LIMIT


def dot(a, b, dims):
    return lax.dot_general(a, b, (dims, ((), ())), preferred_element_type=F32)


NN, NT, TN = ((1,), (0,)), ((1,), (1,)), ((0,), (0,))


def normed(h):
    wide = h.astype(F32)
    scale = lax.rsqrt(jnp.mean(wide * wide, -1, keepdims=True) + 1e-6)
    return (wide * scale).astype(BF16)


def call(body, name, grid, in_specs, out_specs, out_shape, scratch, flops, moved, sends=None, limit=VMEM_LIMIT):
    remote = {} if sends is None else {"collective_id": sends, "has_side_effects": True}
    return pl.pallas_call(
        body,
        grid=grid,
        in_specs=in_specs,
        out_specs=out_specs,
        out_shape=out_shape,
        scratch_shapes=scratch,
        name=name,
        compiler_params=pltpu.CompilerParams(dimension_semantics=("arbitrary",) * len(grid), vmem_limit_bytes=limit, **remote),
        cost_estimate=pl.CostEstimate(flops=flops, bytes_accessed=moved, transcendentals=0),
    )


def once(shape, index):
    return pl.BlockSpec(shape, index, pipeline_mode=pl.Buffered(1))


def shape(dims, dtype):
    return jax.ShapeDtypeStruct(dims, dtype)


class Place:
    def __init__(self):
        s, r = lax.axis_index("s"), lax.axis_index("r")
        self.s, self.r = s, r
        self.x, self.c = s // 2, s % 2
        self.s_core, self.s_x = s + 1 - 2 * self.c, (s + 2) % 4
        self.s_both = (self.s_core + 2) % 4
        self.r_y, self.r_z = (r + 2) % 4, r + 1 - 2 * (r % 2)
        self.r_yz = (self.r_z + 2) % 4
        self.core, self.over_x = {"s": self.s_core}, {"s": self.s_x}
        self.over_y, self.over_z = {"r": self.r_y}, {"r": self.r_z}

    def meet(self):
        barrier = pltpu.get_barrier_semaphore()
        for one in (self.core, self.over_x, self.over_y, self.over_z):
            pl.semaphore_signal(barrier, inc=1, device_id=one, device_id_type=MESH)
        pl.semaphore_wait(barrier, 4)


def remote(src, dst, send, recv, device):
    return pltpu.make_async_remote_copy(
        src_ref=src, dst_ref=dst, send_sem=send, recv_sem=recv, device_id=device, device_id_type=MESH
    )


class Sum:
    PHASES = 5

    def __init__(self, place, refs, out, square, scratch):
        self.place, self.refs, self.out, self.square = place, refs, out, square
        self.kept, self.got, self.far, self.got_x, self.near, self.got_1, self.pair, self.got_2, self.local, self.send, self.recv = scratch
        half = self.far.shape[0] // 2
        self.top, self.low = pl.ds(0, half), pl.ds(half, half)

    @staticmethod
    def scratch(rows, cols):
        one = lambda *lead: pltpu.VMEM((*lead, rows, cols), BF16)
        sems = [pltpu.SemaphoreType.DMA((k,)) for k in (2, 7, 7)]
        return [one(2), one(2), one(), one(), one(), one(), one(), one(), *sems]

    def copies(self, phase):
        p, over = self.place, lambda i, src, dst, to: remote(src, dst, self.send.at[i], self.recv.at[i], to)
        if phase == 0:
            return [over(i, self.refs[2 + i], self.got.at[i], p.core) for i in range(2)]
        if phase == 1:
            return [over(2, self.far, self.got_x, p.over_x)]
        if phase == 2:
            return [
                over(3, self.near.at[self.top], self.got_1.at[self.top], p.over_y),
                over(4, self.near.at[self.low], self.got_1.at[self.low], p.over_z),
            ]
        return [
            over(5, self.pair.at[self.top], self.got_2.at[self.top], p.over_z),
            over(6, self.pair.at[self.low], self.got_2.at[self.low], p.over_y),
        ]

    def locals(self):
        return [pltpu.make_async_copy(self.refs[i], self.kept.at[i], self.local.at[i]) for i in range(2)]

    def run(self, phase):
        x = self.place.x
        wide = lambda ref: ref.astype(F32)
        if phase == 0:
            for one in self.locals() + self.copies(0):
                one.start()
            return
        for one in self.copies(phase - 1):
            one.wait()
        if phase == 1:
            for one in self.locals():
                one.wait()
            self.far[...] = (wide(self.kept[1 - x]) + wide(self.got[1 - x])).astype(BF16)
        elif phase == 2:
            self.near[...] = (wide(self.kept[x]) + wide(self.got[x]) + wide(self.got_x[...])).astype(BF16)
        elif phase == 3:
            self.pair[...] = (wide(self.near[...]) + wide(self.got_1[...])).astype(BF16)
        else:
            total = (wide(self.pair[...]) + wide(self.got_2[...])).astype(BF16)
            self.out[...] = total
            self.square[...] = jnp.full(self.square.shape, jnp.sum(wide(total) * wide(total)), F32)
            return
        for one in self.copies(phase):
            one.start()


class Load:
    def __init__(self, terms, id):
        self.terms, self.id = terms, id
        self.sizes = [one[0].shape for one in terms]
        self.args = [ref for one in terms for ref in one]
        self.in_specs = [pl.BlockSpec(memory_space=pl.ANY)] * len(self.args)
        here = lambda *_: (0, 0)
        self.out_specs = [once(size, here) for one in self.sizes for size in (one, (8, 128))]
        self.out_shape = [shape(size, dtype) for one in self.sizes for size, dtype in ((one, BF16), ((8, 128), F32))]
        self.scratch = [ref for size in self.sizes for ref in Sum.scratch(*size)]

    def sums(self, place, ins, outs, scratch):
        per = len(scratch) // len(self.sizes)
        return [
            Sum(place, ins[4 * i : 4 * i + 4], outs[2 * i], outs[2 * i + 1], scratch[per * i : per * i + per])
            for i in range(len(self.sizes))
        ]

    def drive(self, place, sums, step, at):
        for phase, when in enumerate(at):

            @pl.when(step == when)
            def _(phase=phase):
                if phase == 0:
                    place.meet()
                for one in sums:
                    one.run(phase)

    def results(self, outs):
        return list(zip(outs[0::2], outs[1::2]))


def carried(body, load, own_in, own_out, at):
    if load is None:
        return body

    def both(*refs):
        n_in, n_out, n_scratch = len(load.in_specs), len(load.out_specs), len(load.scratch)
        ins, refs = refs[:own_in], refs[own_in:]
        more_in, refs = refs[:n_in], refs[n_in:]
        outs, refs = refs[:own_out], refs[own_out:]
        more_out, refs = refs[:n_out], refs[n_out:]
        scratch, more_scratch = refs[: len(refs) - n_scratch], refs[len(refs) - n_scratch :]
        place = Place()
        load.drive(place, load.sums(place, more_in, more_out, more_scratch), pl.program_id(0), at)
        body(*ins, *outs, *scratch)

    return both


def call_with(load, at, body, name, grid, in_specs, out_specs, out_shape, scratch, flops, moved, args):
    if load is None:
        outs = call(body, name, grid, in_specs, out_specs, out_shape, scratch, flops, moved)(*args)
        return list(outs), []
    outs = call(
        carried(body, load, len(in_specs), len(out_specs), at),
        name,
        grid,
        in_specs + load.in_specs,
        out_specs + load.out_specs,
        out_shape + load.out_shape,
        scratch + load.scratch,
        flops,
        moved,
        load.id,
    )(*args, *load.args)
    return list(outs[: len(out_specs)]), load.results(outs[len(out_specs) :])


def spread(acc, rows, refs):
    c = lax.axis_index("s") % 2
    for i, ref in enumerate(refs):
        at = (i % 2) * 2 + (c if i < 2 else 1 - c)
        ref[...] = acc[pl.ds(pl.multiple_of(at * rows, rows), rows), :].astype(BF16)


def spread_shapes(rows, cols, count=4):
    return [shape((rows, cols), BF16)] * count


def spread_specs(rows, cols, count=4):
    return [once((rows, cols), lambda *_: (0, 0))] * count


def clear(step, *refs):
    @pl.when(step == 0)
    def _():
        for ref in refs:
            ref[...] = jnp.zeros_like(ref)


class Fetch:
    COPIES = 9

    def __init__(self, place, own, full, columns, send, recv, local, stage=None):
        self.place, self.own, self.full, self.columns = place, own, full, columns
        self.send, self.recv, self.local, self.stage = send, recv, local, stage

    def part(self, block, quarter=None):
        rows = self.own.shape[0]
        if self.columns is None:
            if quarter is None:
                return self.full.at[pl.ds(pl.multiple_of(block * rows, rows), rows)]
            return self.full.at[pl.ds(pl.multiple_of(block * rows + quarter * (rows // 4), rows // 4), rows // 4)]
        start, width = self.columns
        across = pl.ds(start, width) if quarter is None else pl.ds(pl.multiple_of(start + quarter * (width // 4), 128), width // 4)
        return self.full.at[pl.ds(pl.multiple_of(block * rows, rows), rows), across]

    def mine(self, quarter=None):
        rows = self.own.shape[0]
        if self.columns is None:
            return self.own if quarter is None else self.own.at[pl.ds(pl.multiple_of(quarter * (rows // 4), rows // 4), rows // 4)]
        start, width = self.columns
        across = pl.ds(start, width) if quarter is None else pl.ds(pl.multiple_of(start + quarter * (width // 4), 128), width // 4)
        return self.own.at[:, across]

    def copy(self, i):
        p = self.place
        over = lambda src, dst, to: remote(src, dst, self.send.at[i], self.recv.at[i], to)
        if i == 0:
            return over(self.mine(), self.part(p.s), p.core)
        if i in (1, 2):
            q = p.r if i == 1 else p.r_yz
            return over(self.mine(q), self.part(p.s, q), p.over_x)
        if i in (3, 4):
            return over(self.part(p.s_x, p.r), self.part(p.s_x, p.r), p.over_y if i == 3 else p.over_z)
        q = (p.r, p.r_yz, p.r_y, p.r_z)[i - 5]
        return over(self.part(p.s_x, q), self.part(p.s_x, q), p.core)

    def start(self, *which):
        for i in which:
            self.copy(i).start()

    def arrived(self, i):
        self.copy(i).wait_recv()

    def begin(self):
        self.start(1, 2, 0)
        into = self.stage if self.stage is not None else self.part(self.place.s)
        pltpu.make_async_copy(self.mine(), into, self.local.at[0]).start()

    def relay(self):
        self.arrived(1)
        self.start(3, 4, 5)
        if self.stage is not None:
            pltpu.make_async_copy(self.mine(), self.stage, self.local.at[0]).wait()
            pltpu.make_async_copy(self.stage, self.part(self.place.s), self.local.at[1]).start()

    def hand_over(self):
        self.arrived(2)
        self.start(6)
        self.arrived(3)
        self.start(7)
        self.arrived(4)
        self.start(8)

    def finish(self):
        if self.stage is not None:
            pltpu.make_async_copy(self.stage, self.part(self.place.s), self.local.at[1]).wait()
        else:
            pltpu.make_async_copy(self.mine(), self.part(self.place.s), self.local.at[0]).wait()
        for i in (0, 5, 6, 7, 8):
            self.arrived(i)
        for i in range(self.COPIES):
            self.copy(i).wait_send()


RUN, HEAD = 512, 1024


def project_body(h_ref, *refs):
    own, refs = [ref.at[number] for number in range(2) for ref in refs[:3]], refs[3:]
    gate_ref, up_ref, prod_ref = refs[:3]
    full, refs = refs[3:7], refs[7:]
    a_all, wg, wu, stage_d0, stage_g1, stage_u1, stage_d1, send, recv, local = refs
    run, tile = pl.program_id(0), pl.program_id(1)
    step = run * pl.num_programs(1) + tile
    place = Place()
    ff = wg.shape[1]
    plan = [
        (own[0], wg, (0, HEAD), None),
        (own[1], wu, (0, HEAD), None),
        (own[0], wg, (HEAD, ff - HEAD), None),
        (own[1], wu, (HEAD, ff - HEAD), None),
        (own[2], full[0], None, stage_d0),
        (own[3], full[1], (0, ff), stage_g1),
        (own[4], full[2], (0, ff), stage_u1),
        (own[5], full[3], None, stage_d1),
    ]
    fetches = [
        Fetch(place, mine, whole, columns, send.at[i], recv.at[i], local.at[i], stage) for i, (mine, whole, columns, stage) in enumerate(plan)
    ]

    @pl.when(step == 0)
    def _():
        place.meet()
        a, b, c, d = fetches[:4]
        for one in (a, b):
            one.begin()
        for one in (c, d):
            one.begin()
        for one in (a, b):
            one.relay()
        for one in (a, b):
            one.hand_over()
        for one in (a, b):
            one.finish()

    for when, number, what in (
        (1, 2, "relay"),
        (1, 3, "relay"),
        (1, 4, "begin"),
        (3, 2, "hand_over"),
        (3, 3, "hand_over"),
        (4, 4, "relay"),
        (4, 5, "begin"),
        (5, 4, "hand_over"),
        (7, 2, "finish"),
        (7, 3, "finish"),
        (8, 5, "relay"),
        (8, 6, "begin"),
        (10, 4, "finish"),
        (11, 5, "hand_over"),
        (11, 6, "relay"),
        (11, 7, "begin"),
        (14, 6, "hand_over"),
        (14, 7, "relay"),
        (17, 7, "hand_over"),
        (18, 5, "finish"),
        (18, 6, "finish"),
        (19, 7, "finish"),
    ):

        @pl.when(step == when)
        def _(number=number, what=what):
            getattr(fetches[number], what)()

    rows = h_ref.shape[0]
    mine = pl.ds(pl.multiple_of(tile * rows, rows), rows)

    @pl.when(run == 0)
    def _():
        a_all[mine, :] = normed(h_ref[...])

    a = a_all[mine, :]
    across = pl.ds(pl.multiple_of(run * RUN, RUN), RUN)
    gate = dot(a, wg[:, across], NN)
    up = dot(a, wu[:, across], NN)
    gate_ref[...] = gate
    up_ref[...] = up
    prod_ref[...] = (gate * jax.nn.sigmoid(gate) * up).astype(BF16)


def project(h, weights, tile=1024):
    n, d = h.shape
    ff = weights[0].shape[2]
    sizes = [one.shape[1:] for one in (weights[2], *weights)]
    rows = pl.BlockSpec((tile, RUN), lambda i, j: (j, i))
    hbm = pl.BlockSpec(memory_space=pl.ANY)
    outs = call(
        project_body,
        "project",
        (ff // RUN, n // tile),
        [pl.BlockSpec((tile, d), lambda i, j: (jnp.where(i == 0, j, n // tile - 1), 0))] + [hbm] * 3,
        [rows] * 3 + [hbm] * 4,
        [shape((n, ff), F32), shape((n, ff), F32), shape((n, ff), BF16)]
        + [shape((rows_ * 4, cols), BF16) for rows_, cols in sizes],
        [pltpu.VMEM((n, d), BF16), pltpu.VMEM((d, ff), BF16), pltpu.VMEM((d, ff), BF16)]
        + [pltpu.VMEM(size, BF16) for size in sizes]
        + [pltpu.SemaphoreType.DMA((8, 9)), pltpu.SemaphoreType.DMA((8, 9)), pltpu.SemaphoreType.DMA((8, 2))],
        4 * n * d * ff,
        n * ff * 10,
        0,
    )(h, *weights)
    return outs[:3], outs[3:]


def down_body(h_ref, prod_ref, wd_ref, out_ref):
    out_ref[...] = h_ref[...] + dot(prod_ref[...], wd_ref[...], NN).astype(BF16)


def down(h, prod, wd, tile=512):
    n, d = h.shape
    ff = wd.shape[0]
    rows = lambda width: pl.BlockSpec((tile, width), lambda i: (i, 0))
    return call(
        down_body,
        "down",
        (n // tile,),
        [rows(d), rows(ff), once((ff, d), lambda i: (0, 0))],
        rows(d),
        shape((n, d), BF16),
        [],
        2 * n * d * ff,
        n * ff * 2,
    )(h, prod, wd)


def slopes(gate, up, dprod):
    s = jax.nn.sigmoid(gate)
    silu = gate * s
    return silu, (dprod * silu).astype(BF16), (dprod * up * (s + silu * (1 - s))).astype(BF16)


def last_body(part, h_ref, dy_ref, wg_ref, wu_ref, wd_ref, dgate_ref, dup_ref, *rest):
    outs, (acc_g, acc_u, acc_d) = rest[:10], rest[10:]
    step = pl.program_id(0)
    clear(step, acc_g, acc_u, acc_d)
    a = normed(h_ref[...])
    dy = dy_ref[...]
    a_t, dy_t = a.T, dy.T
    parts = [slice(i, i + part) for i in range(0, wg_ref.shape[1], part)]
    front = lambda at: (dot(a, wg_ref[:, at], NN), dot(a, wu_ref[:, at], NN), dot(dy, wd_ref[at, :], NT))
    ahead = front(parts[0])
    for i, at in enumerate(parts):
        gate, up, dprod = ahead
        if i + 1 < len(parts):
            ahead = front(parts[i + 1])
        silu, dup, dgate = slopes(gate, up, dprod.astype(BF16).astype(F32))
        dgate_ref[:, at] = dgate
        dup_ref[:, at] = dup
        acc_g[:, at] += dot(a_t, dgate, NN)
        acc_u[:, at] += dot(a_t, dup, NN)
        acc_d[:, at] += dot(dy_t, (silu * up).astype(BF16), NN)

    @pl.when(step == pl.num_programs(0) - 1)
    def _():
        rows = acc_g.shape[0] // 4
        spread(acc_g, rows, outs[:4])
        spread(acc_u, rows, outs[4:8])
        c = lax.axis_index("s") % 2
        rows = acc_d.shape[1] // 2
        for core, ref in ((c, outs[8]), (1 - c, outs[9])):
            ref[...] = acc_d[:, pl.ds(pl.multiple_of(core * rows, rows), rows)].T.astype(BF16)


def last(h, dy, wg, wu, wd, run, runs, load=None, at=(), tile=256, part=256):
    n, d = h.shape
    ff = wg.shape[1] // runs
    rows = lambda width: pl.BlockSpec((tile, width), lambda i: (i, 0))
    columns = lambda: once((d, ff), lambda i: (0, run))
    outs, done = call_with(
        load,
        at,
        functools.partial(last_body, part),
        f"last{run}",
        (n // tile,),
        [rows(d), rows(d), columns(), columns(), once((ff, d), lambda i: (run, 0))],
        [rows(ff), rows(ff)] + spread_specs(d // 4, ff, 8) + spread_specs(ff // 2, d, 2),
        [shape((n, ff), BF16)] * 2 + spread_shapes(d // 4, ff, 8) + spread_shapes(ff // 2, d, 2),
        [pltpu.VMEM((d, ff), F32)] * 3,
        12 * n * d * ff,
        n * ff * 4,
        (h, dy, wg, wu, wd),
    )
    return outs[0], outs[1], outs[2:6], outs[6:10], outs[10:12], done


def inward_body(runs, h_ref, by_ref, *rest):
    dgates, dups, (wg_ref, wu_ref, out_ref) = rest[:runs], rest[runs : 2 * runs], rest[2 * runs :]
    ff = dgates[0].shape[1]
    total = lambda parts, w: sum(dot(p[...], w[:, i * ff : (i + 1) * ff], NT) for i, p in enumerate(parts)).astype(BF16)
    da = (total(dgates, wg_ref) + total(dups, wu_ref)).astype(F32)
    wide = h_ref[...].astype(F32)
    scale = lax.rsqrt(jnp.mean(wide * wide, -1, keepdims=True) + 1e-6)
    along = jnp.mean(da * wide, -1, keepdims=True)
    dh = da * scale - wide * (scale * scale * scale * along)
    out_ref[...] = by_ref[...] + dh.astype(BF16)


def inward(h, by, dgates, dups, wg, wu, load=None, at=(), tile=512):
    n, d = h.shape
    ff = wg.shape[1]
    runs = len(dgates)
    rows = lambda width: pl.BlockSpec((tile, width), lambda i: (i, 0))
    outs, done = call_with(
        load,
        at,
        functools.partial(inward_body, runs),
        "inward",
        (n // tile,),
        [rows(d), rows(d)] + [rows(ff // runs)] * (2 * runs) + [once((d, ff), lambda i: (0, 0))] * 2,
        [rows(d)],
        [shape((n, d), BF16)],
        [],
        4 * n * d * ff,
        n * ff * 4,
        (h, by, *dgates, *dups, wg, wu),
    )
    return outs[0], done


def outer_body(by_ref, prod_ref, *rest):
    outs, acc = rest[:4], rest[4]
    step = pl.program_id(0)
    clear(step, acc)
    acc[...] += dot(by_ref[...].T, prod_ref[...], NN)

    @pl.when(step == pl.num_programs(0) - 1)
    def _():
        c = lax.axis_index("s") % 2
        rows = acc.shape[1] // 4
        for i, ref in enumerate(outs):
            block = (i % 2) * 2 + (c if i < 2 else 1 - c)
            ref[...] = acc[:, pl.ds(pl.multiple_of(block * rows, rows), rows)].T.astype(BF16)


def outer(by, prod, load=None, at=(), tile=512):
    n, d = by.shape
    ff = prod.shape[1]
    rows = lambda width: pl.BlockSpec((tile, width), lambda i: (i, 0))
    return call_with(
        load,
        at,
        outer_body,
        "outer",
        (n // tile,),
        [rows(d), rows(ff)],
        spread_specs(ff // 4, d),
        spread_shapes(ff // 4, d),
        [pltpu.VMEM((d, ff), F32)],
        2 * n * d * ff,
        n * ff * 2,
        (by, prod),
    )


def first_body(part, h_ref, by_ref, gate_ref, up_ref, wd_ref, *rest):
    outs, (acc_g, acc_u) = rest[:8], rest[8:]
    step = pl.program_id(0)
    clear(step, acc_g, acc_u)
    a_t = normed(h_ref[...]).T
    by = by_ref[...]
    parts = [slice(i, i + part) for i in range(0, wd_ref.shape[0], part)]
    front = lambda at: dot(by, wd_ref[at, :], NT)
    ahead = front(parts[0])
    for i, at in enumerate(parts):
        dprod = ahead.astype(BF16).astype(F32)
        if i + 1 < len(parts):
            ahead = front(parts[i + 1])
        _, dup, dgate = slopes(gate_ref[:, at], up_ref[:, at], dprod)
        acc_g[:, at] += dot(a_t, dgate, NN)
        acc_u[:, at] += dot(a_t, dup, NN)

    @pl.when(step == pl.num_programs(0) - 1)
    def _():
        rows = acc_g.shape[0] // 4
        spread(acc_g, rows, outs[:4])
        spread(acc_u, rows, outs[4:])


def first(h, by, gate, up, wd, run, width, load=None, at=(), tile=512, part=256):
    n, d = h.shape
    rows = lambda: pl.BlockSpec((tile, d), lambda i: (i, 0))
    kept = lambda: pl.BlockSpec((tile, width), lambda i: (i, run))
    outs, done = call_with(
        load,
        at,
        functools.partial(first_body, part),
        f"first{run}",
        (n // tile,),
        [rows(), rows(), kept(), kept(), once((width, d), lambda i: (run, 0))],
        spread_specs(d // 4, width, 8),
        spread_shapes(d // 4, width, 8),
        [pltpu.VMEM((d, width), F32)] * 2,
        6 * n * d * width,
        n * width * 8,
        (h, by, gate, up, wd),
    )
    return outs[:4], outs[4:], done


def tail_body(count, squares, load, *refs):
    n_in, n_out = len(load.in_specs), len(load.out_specs)
    others, refs = refs[:squares], refs[squares:]
    ins, refs = refs[:n_in], refs[n_in:]
    outs, factor_ref, refs = refs[:n_out], refs[n_out], refs[n_out + 1 :]
    scratch, (mine, got_core, both, got_x, send, recv) = refs[: len(load.scratch)], refs[len(load.scratch) :]
    place = Place()
    sums = load.sums(place, ins, outs, scratch)
    place.meet()
    for wave in range(len(sums) + Sum.PHASES - 1):
        for i, one in enumerate(sums):
            if i == 0 and wave == 0:
                for each in sums:
                    each.run(0)
            if 1 <= wave - i + 1 < Sum.PHASES:
                one.run(wave - i + 1)
    total = sum(ref[...] for ref in others) + sum(one.square[...] for one in sums)
    mine[...] = total
    hop = remote(mine, got_core, send.at[0], recv.at[0], place.core)
    hop.start()
    hop.wait()
    both[...] = mine[...] + got_core[...]
    hop = remote(both, got_x, send.at[1], recv.at[1], place.over_x)
    hop.start()
    hop.wait()
    factor_ref[...] = jnp.minimum(1.0, 0.5 * lax.rsqrt((both[...] + got_x[...]) / count + 1e-30))


def tail(load, squares, count):
    whole = pl.BlockSpec((8, 128), lambda: (0, 0))
    outs = call(
        functools.partial(tail_body, count, len(squares), load),
        "tail",
        (),
        [whole] * len(squares) + load.in_specs,
        [pl.BlockSpec(one.block_shape, lambda: (0, 0)) for one in load.out_specs] + [whole],
        load.out_shape + [shape((8, 128), F32)],
        load.scratch + [pltpu.VMEM((8, 128), F32)] * 4 + [pltpu.SemaphoreType.DMA((2,))] * 2,
        1000,
        1000,
        load.id,
        SMALL,
    )(*squares, *load.args)
    return load.results(outs[:-1]), outs[-1]


def adamw(w, m, v, g):
    m = 0.9 * m + 0.1 * g
    v = 0.95 * v + 0.05 * g * g
    step = m * lax.rsqrt(v + 1e-8) + 0.1 * w
    return (w - 0.02 * step).astype(BF16), m, v


def update_body(edges, factor_ref, *refs):
    counts = [[len(e) - 1 for e in one] for one in edges]
    total = sum(map(sum, counts))
    grads, refs = refs[:total], refs[total:]
    states, news = refs[:9], refs[9:]
    layer, turn = pl.program_id(0), pl.program_id(1)
    factor = factor_ref[0, 0]
    k = 0
    for i, per_layer in enumerate(edges):
        for number, edge in enumerate(per_layer):
            for low, high in zip(edge, edge[1:]):

                @pl.when((layer == number) & (turn >= low) & (turn < high))
                def _(ref=grads[k], i=i):
                    w, m, v = (states[3 * which + i][0] for which in range(3))
                    for which, one in enumerate(adamw(w.astype(F32), m, v, ref[...].astype(F32) * factor)):
                        news[3 * which + i][0] = one

                k += 1


def update(factor, pieces, states, turns=10):
    specs, edges, args = [pl.BlockSpec(memory_space=pltpu.SMEM)], [], [factor]
    state_specs = []
    for i, per_layer in enumerate(pieces):
        _, rows, cols = states[i].shape
        tall = i == 2
        block = (rows // turns, cols) if tall else (rows, cols // turns)
        edges.append([])
        for number, parts in enumerate(per_layer):
            edge = [0]
            for part in parts:
                low = edge[-1]
                edge.append(low + (part.shape[0] // block[0] if tall else part.shape[1] // block[1]))

                def index(layer, turn, number=number, low=low, top=edge[-1] - low - 1, tall=tall):
                    at = jnp.where(layer == number, jnp.clip(turn - low, 0, top), jnp.where(layer < number, 0, top))
                    return (at, 0) if tall else (0, at)

                specs.append(pl.BlockSpec(block, index))
                args.append(part)
            edges[-1].append(edge)
        state_specs.append(pl.BlockSpec((1, *block), (lambda layer, turn: (layer, turn, 0)) if tall else (lambda layer, turn: (layer, 0, turn))))
    return call(
        functools.partial(update_body, edges),
        "update",
        (2, turns),
        specs + state_specs * 3,
        state_specs * 3,
        [shape(one.shape, one.dtype) for one in states],
        [],
        1000000,
        1000000,
        limit=SMALL,
    )(*args, *states)


def solution(mesh):
    ns = mesh.shape["s"]

    def step(x, dy, *arrays):
        weights, m, v = (arrays[i : i + 3] for i in (0, 3, 6))
        h0, dy = x[0], dy[0]
        (gate, up, prod), (wd0, wg1, wu1, wd1) = project(h0, weights)
        h1 = down(h0, prod, wd0)
        a = last(h1, dy, wg1, wu1, wd1, 0, 2)
        b = last(h1, dy, wg1, wu1, wd1, 1, 2, Load([a[2], a[3]], 1), (0, 2, 6, 9, 12))
        (g1a, u1a) = b[5]
        by, (g1b, u1b) = inward(h1, dy, [a[0], b[0]], [a[1], b[1]], wg1, wu1, Load([b[2], b[3]], 2), (0, 1, 5, 6, 7))
        d0, (d1,) = outer(by, prod, Load([[a[4][0], b[4][0], a[4][1], b[4][1]]], 3), (0, 1, 5, 6, 7))
        c = first(h0, by, gate, up, wd0, 0, 1280, Load([d0], 4), (0, 1, 5, 6, 7))
        (d0,) = c[2]
        e = first(h0, by, gate, up, wd0, 1, 1280, Load([c[0], c[1]], 5), (0, 1, 5, 6, 7))
        g0a, u0a = e[2]
        done = [g1a, u1a, g1b, u1b, d1, d0, g0a, u0a]
        count = ns * sum(w.size for w in weights)
        (g0b, u0b), factor = tail(Load([e[0], e[1]], 6), [one[1] for one in done], count)
        parts = lambda *ones: [one[0] for one in ones]
        pieces = [
            [parts(g0a, g0b), parts(g1a, g1b)],
            [parts(u0a, u0b), parts(u1a, u1b)],
            [parts(d0), parts(d1)],
        ]
        return tuple(update(factor, pieces, [*weights, *m, *v]))

    states, cut = P(("rep", "r", "s"), None, None), P(None, "s", None)
    return jax.shard_map(
        step,
        mesh=mesh,
        in_specs=(states, states) + (cut,) * 9,
        out_specs=(P("rep", "s", None),) * 9,
        check_vma=False,
    )
```

```python
import functools
import math

import jax
import jax.numpy as jnp
from jax import lax
from jax.experimental import pallas as pl
from jax.experimental.pallas import tpu as pltpu
from jax.sharding import PartitionSpec as P

NAMES = ("w_gate", "w_up", "w_down")
F32, BF16 = jnp.float32, jnp.bfloat16
MESH = pl.DeviceIdType.MESH
VMEM_LIMIT = 60 * 1024 * 1024
SMALL = VMEM_LIMIT


def dot(a, b, dims):
    return lax.dot_general(a, b, (dims, ((), ())), preferred_element_type=F32)


NN, NT, TN = ((1,), (0,)), ((1,), (1,)), ((0,), (0,))


def normed(h):
    wide = h.astype(F32)
    scale = lax.rsqrt(jnp.mean(wide * wide, -1, keepdims=True) + 1e-6)
    return (wide * scale).astype(BF16)


def call(body, name, grid, in_specs, out_specs, out_shape, scratch, flops, moved, sends=None, limit=VMEM_LIMIT):
    remote = {} if sends is None else {"collective_id": sends, "has_side_effects": True}
    return pl.pallas_call(
        body,
        grid=grid,
        in_specs=in_specs,
        out_specs=out_specs,
        out_shape=out_shape,
        scratch_shapes=scratch,
        name=name,
        compiler_params=pltpu.CompilerParams(dimension_semantics=("arbitrary",) * len(grid), vmem_limit_bytes=limit, **remote),
        cost_estimate=pl.CostEstimate(flops=flops, bytes_accessed=moved, transcendentals=0),
    )


def once(shape, index):
    return pl.BlockSpec(shape, index, pipeline_mode=pl.Buffered(1))


def shape(dims, dtype):
    return jax.ShapeDtypeStruct(dims, dtype)


class Place:
    def __init__(self):
        s, r = lax.axis_index("s"), lax.axis_index("r")
        self.s, self.r = s, r
        self.x, self.c = s // 2, s % 2
        self.s_core, self.s_x = s + 1 - 2 * self.c, (s + 2) % 4
        self.s_both = (self.s_core + 2) % 4
        self.r_y, self.r_z = (r + 2) % 4, r + 1 - 2 * (r % 2)
        self.r_yz = (self.r_z + 2) % 4
        self.core, self.over_x = {"s": self.s_core}, {"s": self.s_x}
        self.over_y, self.over_z = {"r": self.r_y}, {"r": self.r_z}

    def meet(self):
        barrier = pltpu.get_barrier_semaphore()
        for one in (self.core, self.over_x, self.over_y, self.over_z):
            pl.semaphore_signal(barrier, inc=1, device_id=one, device_id_type=MESH)
        pl.semaphore_wait(barrier, 4)


def remote(src, dst, send, recv, device):
    return pltpu.make_async_remote_copy(
        src_ref=src, dst_ref=dst, send_sem=send, recv_sem=recv, device_id=device, device_id_type=MESH
    )


class Sum:
    FIRST = {"all": 0, "x": 0, "yz": 2}
    LAST = {"all": 4, "x": 2, "yz": 4}

    def __init__(self, place, kind, refs, outs, scratch):
        self.place, self.kind, self.refs, self.out = place, kind, refs, outs[0]
        self.square = outs[1] if kind != "x" else None
        self.local, self.send, self.recv = scratch[-3:]
        scratch = scratch[:-3]
        if kind != "yz":
            self.kept, self.got, self.far, self.got_x = scratch[:4]
            scratch = scratch[4:]
        if kind != "x":
            self.near, self.got_1, self.pair, self.got_2 = scratch
        half = self.out.shape[0] // 2
        self.top, self.low = pl.ds(0, half), pl.ds(half, half)

    @staticmethod
    def scratch(kind, rows, cols):
        one = lambda *lead: pltpu.VMEM((*lead, rows, cols), BF16)
        to_x = [one(2), one(2), one(), one()] if kind != "yz" else []
        to_yz = [one()] * 4 if kind != "x" else []
        return to_x + to_yz + [pltpu.SemaphoreType.DMA((k,)) for k in (2, 7, 7)]

    def copies(self, phase):
        p, over = self.place, lambda i, src, dst, to: remote(src, dst, self.send.at[i], self.recv.at[i], to)
        if phase == 0:
            return [over(i, self.refs[2 + i], self.got.at[i], p.core) for i in range(2)]
        if phase == 1:
            return [over(2, self.far, self.got_x, p.over_x)]
        if phase == 2:
            return [
                over(3, self.near.at[self.top], self.got_1.at[self.top], p.over_y),
                over(4, self.near.at[self.low], self.got_1.at[self.low], p.over_z),
            ]
        return [
            over(5, self.pair.at[self.top], self.got_2.at[self.top], p.over_z),
            over(6, self.pair.at[self.low], self.got_2.at[self.low], p.over_y),
        ]

    def locals(self):
        if self.kind == "yz":
            return [pltpu.make_async_copy(self.refs[0], self.near, self.local.at[0])]
        return [pltpu.make_async_copy(self.refs[i], self.kept.at[i], self.local.at[i]) for i in range(2)]

    def run(self, phase):
        x = self.place.x
        wide = lambda ref: ref.astype(F32)
        if phase == 0:
            for one in self.locals() + self.copies(0):
                one.start()
            return
        if phase == 2 and self.kind == "yz":
            for one in self.locals():
                one.start()
                one.wait()
        else:
            for one in self.copies(phase - 1):
                one.wait()
        if phase == 1:
            for one in self.locals():
                one.wait()
            self.far[...] = (wide(self.kept[1 - x]) + wide(self.got[1 - x])).astype(BF16)
        elif phase == 2 and self.kind != "yz":
            into = self.out if self.kind == "x" else self.near
            into[...] = (wide(self.kept[x]) + wide(self.got[x]) + wide(self.got_x[...])).astype(BF16)
        elif phase == 3:
            self.pair[...] = (wide(self.near[...]) + wide(self.got_1[...])).astype(BF16)
        elif phase == 4:
            total = (wide(self.pair[...]) + wide(self.got_2[...])).astype(BF16)
            self.out[...] = total
            self.square[...] = jnp.full(self.square.shape, jnp.sum(wide(total) * wide(total)), F32)
        if phase < Sum.LAST[self.kind]:
            for one in self.copies(phase):
                one.start()


def timeline(sizes, kinds, steps, step_us):
    rate = {"core": 4e5, "x": 4.6e4, "y": 4.6e4, "z": 4.6e4}
    free = dict.fromkeys(rate, 0.0)
    parts = {0: (("core", 2.0),), 1: (("x", 1.0),), 2: (("y", 0.5), ("z", 0.5)), 3: (("y", 0.5), ("z", 0.5))}
    phase = [Sum.FIRST[kind] for kind in kinds]
    ready, order, now, k = [0.0] * len(sizes), [], 0.0, 0
    while any(p <= Sum.LAST[kind] for p, kind in zip(phase, kinds)):
        waiting = [i for i, kind in enumerate(kinds) if phase[i] <= Sum.LAST[kind]]
        able = [i for i in waiting if ready[i] <= now]
        if not able and k < steps:
            k += 1
            now = max(now, k * step_us)
            continue
        i = min(able or waiting, key=lambda j: (ready[j], -phase[j], j))
        now = max(now, ready[i])
        order.append((k, i, phase[i]))
        ends = [now]
        for link, share in parts.get(phase[i], ()):
            free[link] = max(free[link], now) + share * sizes[i][0] * sizes[i][1] * 2 / rate[link]
            ends.append(free[link] + 2.0)
        ready[i] = max(ends)
        phase[i] += 1
    return order


class Load:
    def __init__(self, id, jobs):
        self.id = id
        self.kinds = [kind for kind, _, _ in jobs]
        self.parts = [part for _, _, part in jobs]
        self.sizes = [
            tuple(part[2] if part and part[0] == i else size for i, size in enumerate(terms[0].shape)) for _, terms, part in jobs
        ]
        self.counts = [len(terms) for _, terms, _ in jobs]
        self.args = [ref for _, terms, _ in jobs for ref in terms]
        self.in_specs = [pl.BlockSpec(memory_space=pl.ANY)] * len(self.args)
        here = lambda *_: (0, 0)
        results = [
            each for size, kind in zip(self.sizes, self.kinds) for each in [(size, BF16)] + ([] if kind == "x" else [((8, 128), F32)])
        ]
        self.out_specs = [once(size, here) for size, _ in results]
        self.out_shape = [shape(size, dtype) for size, dtype in results]
        self.scratch = [ref for size, kind in zip(self.sizes, self.kinds) for ref in Sum.scratch(kind, *size)]

    def sums(self, place, ins, outs, scratch):
        made = []
        for kind, part, size, count in zip(self.kinds, self.parts, self.sizes, self.counts):
            terms, ins = ins[:count], ins[count:]
            if part is not None:
                at = pl.ds(*part[1:])
                terms = [ref.at[at] if part[0] == 0 else ref.at[:, at] for ref in terms]
            n = 1 if kind == "x" else 2
            m = len(Sum.scratch(kind, *size))
            made.append(Sum(place, kind, terms, outs[:n], scratch[:m]))
            outs, scratch = outs[n:], scratch[m:]
        return made

    def results(self, outs):
        made = []
        for kind in self.kinds:
            n = 1 if kind == "x" else 2
            made.append(outs[0] if n == 1 else (outs[0], outs[1]))
            outs = outs[n:]
        return made


def carried(body, load, own_in, own_out, steps, step_us):
    order = timeline(load.sizes, load.kinds, steps, step_us)

    def both(*refs):
        n_in, n_out, n_scratch = len(load.in_specs), len(load.out_specs), len(load.scratch)
        ins, refs = refs[:own_in], refs[own_in:]
        more_in, refs = refs[:n_in], refs[n_in:]
        outs, refs = refs[:own_out], refs[own_out:]
        more_out, refs = refs[:n_out], refs[n_out:]
        scratch, more_scratch = refs[: len(refs) - n_scratch], refs[len(refs) - n_scratch :]
        place = Place()
        step = pl.program_id(0)
        sums = load.sums(place, more_in, more_out, more_scratch)

        def act(at):
            todo = [(i, phase) for when, i, phase in order if when == at]
            if todo:

                @pl.when(step == min(at, steps - 1))
                def _():
                    if at == 0:
                        place.meet()
                    for i, phase in todo:
                        sums[i].run(phase)

        for at in range(steps):
            act(at)
        body(*ins, *outs, *scratch)
        act(steps)

    return both


def call_with(load, step_us, body, name, grid, in_specs, out_specs, out_shape, scratch, flops, moved, args):
    if load is None:
        outs = call(body, name, grid, in_specs, out_specs, out_shape, scratch, flops, moved)(*args)
        return list(outs), []
    outs = call(
        carried(body, load, len(in_specs), len(out_specs), grid[0], step_us),
        name,
        grid,
        in_specs + load.in_specs,
        out_specs + load.out_specs,
        out_shape + load.out_shape,
        scratch + load.scratch,
        flops,
        moved,
        load.id,
    )(*args, *load.args)
    return list(outs[: len(out_specs)]), load.results(outs[len(out_specs) :])


def spread(acc, rows, refs):
    c = lax.axis_index("s") % 2
    for i, ref in enumerate(refs):
        at = (i % 2) * 2 + (c if i < 2 else 1 - c)
        ref[...] = acc[pl.ds(pl.multiple_of(at * rows, rows), rows), :].astype(BF16)


def spread_shapes(rows, cols, count=4):
    return [shape((rows, cols), BF16)] * count


def spread_specs(rows, cols, count=4):
    return [once((rows, cols), lambda *_: (0, 0))] * count


def clear(step, *refs):
    @pl.when(step == 0)
    def _():
        for ref in refs:
            ref[...] = jnp.zeros_like(ref)


class Fetch:
    COPIES = 9

    def __init__(self, place, own, full, columns, send, recv, local, stage=None, last="x"):
        self.place, self.own, self.full, self.columns = place, own, full, columns
        self.send, self.recv, self.local, self.stage, self.last = send, recv, local, stage, last

    def part(self, block, quarter=None):
        rows = self.own.shape[0]
        if self.columns is None:
            if quarter is None:
                return self.full.at[pl.ds(pl.multiple_of(block * rows, rows), rows)]
            return self.full.at[pl.ds(pl.multiple_of(block * rows + quarter * (rows // 4), rows // 4), rows // 4)]
        start, width = self.columns
        across = pl.ds(start, width) if quarter is None else pl.ds(pl.multiple_of(start + quarter * (width // 4), 128), width // 4)
        return self.full.at[pl.ds(pl.multiple_of(block * rows, rows), rows), across]

    def mine(self, quarter=None):
        rows = self.own.shape[0]
        if self.columns is None:
            return self.own if quarter is None else self.own.at[pl.ds(pl.multiple_of(quarter * (rows // 4), rows // 4), rows // 4)]
        start, width = self.columns
        across = pl.ds(start, width) if quarter is None else pl.ds(pl.multiple_of(start + quarter * (width // 4), 128), width // 4)
        return self.own.at[:, across]

    def copy(self, i):
        p = self.place
        over = lambda src, dst, to: remote(src, dst, self.send.at[i], self.recv.at[i], to)
        if i == 0:
            return over(self.mine(), self.part(p.s), p.core)
        if i == 1 or (i == 2 and self.last == "x"):
            q = p.r if i == 1 else p.r_yz
            return over(self.mine(q), self.part(p.s, q), p.over_x)
        if i == 2:
            q, to = (p.r_z, p.over_y) if self.last == "y" else (p.r_y, p.over_z)
            return over(self.part(p.s_x, q), self.part(p.s_x, q), to)
        if i in (3, 4):
            return over(self.part(p.s_x, p.r), self.part(p.s_x, p.r), p.over_y if i == 3 else p.over_z)
        q = (p.r, p.r_yz, p.r_y, p.r_z)[i - 5]
        return over(self.part(p.s_x, q), self.part(p.s_x, q), p.core)

    def received(self, i):
        p = self.place
        if i == 0:
            return self.part(p.s_core)
        block, q = [(p.s_x, p.r), (p.s_x, p.r_yz), (p.s_x, p.r_y), (p.s_x, p.r_z)][i - 1] if i < 5 else (p.s_both, (p.r, p.r_yz, p.r_y, p.r_z)[i - 5])
        return self.part(block, q)

    def start(self, *which):
        for i in which:
            self.copy(i).start()

    def arrived(self, i):
        here = self.received(i)
        remote(here, here, self.send.at[i], self.recv.at[i], self.place.core).wait_recv()

    def begin(self):
        self.start(1, *((2,) if self.last == "x" else ()), 0)
        into = self.stage if self.stage is not None else self.part(self.place.s)
        pltpu.make_async_copy(self.mine(), into, self.local.at[0]).start()

    def relay(self):
        self.arrived(1)
        self.start(3, 4, 5)
        if self.stage is not None:
            pltpu.make_async_copy(self.mine(), self.stage, self.local.at[0]).wait()
            pltpu.make_async_copy(self.stage, self.part(self.place.s), self.local.at[1]).start()

    def hand_over(self):
        self.arrived(3)
        self.start(7, *((2,) if self.last == "z" else ()))
        self.arrived(4)
        self.start(8, *((2,) if self.last == "y" else ()))

    def hand_last(self):
        self.arrived(2)
        self.start(6)

    def finish(self):
        if self.stage is not None:
            pltpu.make_async_copy(self.stage, self.part(self.place.s), self.local.at[1]).wait()
        else:
            pltpu.make_async_copy(self.mine(), self.part(self.place.s), self.local.at[0]).wait()
        for i in (0, 5, 6, 7, 8):
            self.arrived(i)
        for i in range(self.COPIES):
            self.copy(i).wait_send()


RUN, HEAD = 512, 1024


def project_body(h_ref, *refs):
    g, u, d, refs = *refs[:3], refs[3:]
    gate_ref, up_ref, prod_ref = refs[:3]
    full, refs = refs[3:6], refs[6:]
    a_all, wg, wu, stage_d0, stage_g1, stage_u1, send, recv, local = refs
    run, tile = pl.program_id(0), pl.program_id(1)
    step = run * pl.num_programs(1) + tile
    place = Place()
    ff = wg.shape[1]
    plan = [
        (g.at[0], wg, (0, HEAD), None, "x"),
        (u.at[0], wu, (0, HEAD), None, "x"),
        (g.at[0], wg, (HEAD, ff - HEAD), None, "x"),
        (u.at[0], wu, (HEAD, ff - HEAD), None, "x"),
        (d.at[0], full[0], None, stage_d0, "x"),
        (g.at[1], full[1], (0, ff), stage_g1, "y"),
        (u.at[1], full[2], (0, ff), stage_u1, "x"),
    ]
    fetches = [
        Fetch(place, mine, whole, columns, send.at[i], recv.at[i], local.at[i], stage, last)
        for i, (mine, whole, columns, stage, last) in enumerate(plan)
    ]

    def act(moves):
        for when, number, what in moves:

            @pl.when(step == when)
            def _(number=number, what=what):
                getattr(fetches[number], what)()

    @pl.when(step == 0)
    def _():
        place.meet()
        a, b, c, d = fetches[:4]
        for one in (a, b, c, d):
            one.begin()
        for what in ("relay", "hand_over", "hand_last", "finish"):
            for one in (a, b):
                getattr(one, what)()

    act(
        (
            (1, 2, "relay"),
            (4, 3, "relay"),
            (4, 2, "hand_over"),
            (4, 2, "hand_last"),
            (4, 4, "begin"),
            (6, 3, "hand_over"),
            (6, 3, "hand_last"),
            (6, 5, "begin"),
            (7, 2, "finish"),
            (7, 3, "finish"),
            (8, 4, "relay"),
            (8, 6, "begin"),
            (11, 4, "hand_over"),
            (11, 4, "hand_last"),
            (12, 5, "relay"),
            (14, 4, "finish"),
            (15, 5, "hand_over"),
            (15, 6, "relay"),
            (18, 5, "hand_last"),
        )
    )
    rows = h_ref.shape[0]
    mine = pl.ds(pl.multiple_of(tile * rows, rows), rows)

    @pl.when(run == 0)
    def _():
        a_all[mine, :] = normed(h_ref[...])

    a = a_all[mine, :]
    part = RUN // 2
    front = lambda i: [
        dot(a, w[:, pl.ds(pl.multiple_of(run * RUN + i * part, part), part)], NN) for w in (wg, wu)
    ]
    ahead = front(0)
    for i in range(2):
        gate, up = ahead
        if i == 0:
            ahead = front(1)
        at = slice(i * part, (i + 1) * part)
        gate_ref[:, at] = gate
        up_ref[:, at] = up
        prod_ref[:, at] = (gate * jax.nn.sigmoid(gate) * up).astype(BF16)
    act(((19, 6, "hand_over"), (19, 6, "hand_last"), (19, 5, "finish"), (19, 6, "finish")))


def project(h, weights, tile=1024):
    n, d = h.shape
    ff = weights[0].shape[2]
    sizes = [one.shape[1:] for one in (weights[2], *weights[:2])]
    rows = pl.BlockSpec((tile, RUN), lambda i, j: (j, i))
    hbm = pl.BlockSpec(memory_space=pl.ANY)
    outs = call(
        project_body,
        "project",
        (ff // RUN, n // tile),
        [pl.BlockSpec((tile, d), lambda i, j: (jnp.where(i == 0, j, n // tile - 1), 0))] + [hbm] * 3,
        [rows] * 3 + [hbm] * 3,
        [shape((n, ff), F32), shape((n, ff), F32), shape((n, ff), BF16)]
        + [shape((high * 4, cols), BF16) for high, cols in sizes],
        [pltpu.VMEM((n, d), BF16), pltpu.VMEM((d, ff), BF16), pltpu.VMEM((d, ff), BF16)]
        + [pltpu.VMEM(size, BF16) for size in sizes]
        + [pltpu.SemaphoreType.DMA((7, 9)), pltpu.SemaphoreType.DMA((7, 9)), pltpu.SemaphoreType.DMA((7, 2))],
        4 * n * d * ff,
        n * ff * 10,
        0,
    )(h, *weights)
    return outs[:3], outs[3:]


def down_body(h_ref, prod_ref, wd_ref, d_ref, out_ref, full, stage, send, recv, local):
    step = pl.program_id(0)
    place = Place()
    fetch = Fetch(place, d_ref.at[1], full, None, send, recv, local, stage)

    def act(when, *what):
        @pl.when(step == when)
        def _():
            if when == 0:
                place.meet()
            for one in what:
                getattr(fetch, one)()

    act(0, "begin")
    act(3, "relay")
    act(5, "hand_over", "hand_last")
    out_ref[...] = h_ref[...] + dot(prod_ref[...], wd_ref[...], NN).astype(BF16)
    act(pl.num_programs(0) - 1, "finish")


def down(h, prod, wd, w_down, tile=512):
    n, d = h.shape
    ff = wd.shape[0]
    rows = lambda width: pl.BlockSpec((tile, width), lambda i: (i, 0))
    hbm = pl.BlockSpec(memory_space=pl.ANY)
    return call(
        down_body,
        "down",
        (n // tile,),
        [rows(d), rows(ff), once((ff, d), lambda i: (0, 0)), hbm],
        [rows(d), hbm],
        [shape((n, d), BF16), shape((ff, d), BF16)],
        [pltpu.VMEM(w_down.shape[1:], BF16), pltpu.SemaphoreType.DMA((9,)), pltpu.SemaphoreType.DMA((9,)), pltpu.SemaphoreType.DMA((2,))],
        2 * n * d * ff,
        n * ff * 2,
        7,
    )(h, prod, wd, w_down)


def slopes(gate, up, dprod):
    s = jax.nn.sigmoid(gate)
    silu = gate * s
    return silu, (dprod * silu).astype(BF16), (dprod * up * (s + silu * (1 - s))).astype(BF16)


def last_body(part, h_ref, dy_ref, wg_ref, wu_ref, wd_ref, dgate_ref, dup_ref, *rest):
    outs, (acc_g, acc_u, acc_d) = rest[:10], rest[10:]
    step = pl.program_id(0)
    clear(step, acc_g, acc_u, acc_d)
    a = normed(h_ref[...])
    dy = dy_ref[...]
    a_t, dy_t = a.T, dy.T
    parts = [slice(i, i + part) for i in range(0, wg_ref.shape[1], part)]
    front = lambda at: (dot(a, wg_ref[:, at], NN), dot(a, wu_ref[:, at], NN), dot(dy, wd_ref[at, :], NT))
    ahead = front(parts[0])
    for i, at in enumerate(parts):
        gate, up, dprod = ahead
        if i + 1 < len(parts):
            ahead = front(parts[i + 1])
        silu, dup, dgate = slopes(gate, up, dprod.astype(BF16).astype(F32))
        dgate_ref[:, at] = dgate
        dup_ref[:, at] = dup
        acc_g[:, at] += dot(a_t, dgate, NN)
        acc_u[:, at] += dot(a_t, dup, NN)
        acc_d[:, at] += dot(dy_t, (silu * up).astype(BF16), NN)

    @pl.when(step == pl.num_programs(0) - 1)
    def _():
        rows = acc_g.shape[0] // 4
        spread(acc_g, rows, outs[:4])
        spread(acc_u, rows, outs[4:8])
        c = lax.axis_index("s") % 2
        rows = acc_d.shape[1] // 2
        for core, ref in ((c, outs[8]), (1 - c, outs[9])):
            ref[...] = acc_d[:, pl.ds(pl.multiple_of(core * rows, rows), rows)].T.astype(BF16)


def last(h, dy, wg, wu, wd, run, runs, load=None, step_us=1.0, tile=512, part=256):
    n, d = h.shape
    ff = wg.shape[1] // runs
    rows = lambda width: pl.BlockSpec((tile, width), lambda i: (i, 0))
    columns = lambda: once((d, ff), lambda i: (0, run))
    outs, done = call_with(
        load,
        step_us,
        functools.partial(last_body, part),
        f"last{run}",
        (n // tile,),
        [rows(d), rows(d), columns(), columns(), once((ff, d), lambda i: (run, 0))],
        [rows(ff), rows(ff)] + spread_specs(d // 4, ff, 8) + spread_specs(ff // 2, d, 2),
        [shape((n, ff), BF16)] * 2 + spread_shapes(d // 4, ff, 8) + spread_shapes(ff // 2, d, 2),
        [pltpu.VMEM((d, ff), F32)] * 3,
        12 * n * d * ff,
        n * ff * 4,
        (h, dy, wg, wu, wd),
    )
    return outs[0], outs[1], outs[2:6], outs[6:10], outs[10:12], done


def inward_body(runs, h_ref, by_ref, *rest):
    dgates, dups, (wg_ref, wu_ref, out_ref) = rest[:runs], rest[runs : 2 * runs], rest[2 * runs :]
    ff = dgates[0].shape[1]
    total = lambda parts, w: sum(dot(p[...], w[:, i * ff : (i + 1) * ff], NT) for i, p in enumerate(parts)).astype(BF16)
    da = (total(dgates, wg_ref) + total(dups, wu_ref)).astype(F32)
    wide = h_ref[...].astype(F32)
    scale = lax.rsqrt(jnp.mean(wide * wide, -1, keepdims=True) + 1e-6)
    along = jnp.mean(da * wide, -1, keepdims=True)
    dh = da * scale - wide * (scale * scale * scale * along)
    out_ref[...] = by_ref[...] + dh.astype(BF16)


def inward(h, by, dgates, dups, wg, wu, load=None, step_us=1.0, tile=512):
    n, d = h.shape
    ff = wg.shape[1]
    runs = len(dgates)
    rows = lambda width: pl.BlockSpec((tile, width), lambda i: (i, 0))
    outs, done = call_with(
        load,
        step_us,
        functools.partial(inward_body, runs),
        "inward",
        (n // tile,),
        [rows(d), rows(d)] + [rows(ff // runs)] * (2 * runs) + [once((d, ff), lambda i: (0, 0))] * 2,
        [rows(d)],
        [shape((n, d), BF16)],
        [],
        4 * n * d * ff,
        n * ff * 4,
        (h, by, *dgates, *dups, wg, wu),
    )
    return outs[0], done


def outer_body(by_ref, prod_ref, *rest):
    outs, acc = rest[:4], rest[4]
    step = pl.program_id(0)
    clear(step, acc)
    acc[...] += dot(by_ref[...].T, prod_ref[...], NN)

    @pl.when(step == pl.num_programs(0) - 1)
    def _():
        c = lax.axis_index("s") % 2
        rows = acc.shape[1] // 4
        for i, ref in enumerate(outs):
            block = (i % 2) * 2 + (c if i < 2 else 1 - c)
            ref[...] = acc[:, pl.ds(pl.multiple_of(block * rows, rows), rows)].T.astype(BF16)


def outer(by, prod, load=None, step_us=1.0, tile=512):
    n, d = by.shape
    ff = prod.shape[1]
    rows = lambda width: pl.BlockSpec((tile, width), lambda i: (i, 0))
    return call_with(
        load,
        step_us,
        outer_body,
        "outer",
        (n // tile,),
        [rows(d), rows(ff)],
        spread_specs(ff // 4, d),
        spread_shapes(ff // 4, d),
        [pltpu.VMEM((d, ff), F32)],
        2 * n * d * ff,
        n * ff * 2,
        (by, prod),
    )


def first_body(part, blocks, h_ref, by_ref, *rest):
    gates, ups, wds, rest = rest[:blocks], rest[blocks : 2 * blocks], rest[2 * blocks : 3 * blocks], rest[3 * blocks :]
    outs, (acc_g, acc_u) = rest[:8], rest[8:]
    step = pl.program_id(0)
    clear(step, acc_g, acc_u)
    a_t = normed(h_ref[...]).T
    by = by_ref[...]
    width = wds[0].shape[0]
    parts = [(k, slice(i, i + part)) for k in range(blocks) for i in range(0, width, part)]
    front = lambda k, at: dot(by, wds[k][at, :], NT)
    ahead = front(*parts[0])
    for i, (k, at) in enumerate(parts):
        dprod = ahead.astype(BF16).astype(F32)
        if i + 1 < len(parts):
            ahead = front(*parts[i + 1])
        _, dup, dgate = slopes(gates[k][:, at], ups[k][:, at], dprod)
        to = slice(i * part, (i + 1) * part)
        acc_g[:, to] += dot(a_t, dgate, NN)
        acc_u[:, to] += dot(a_t, dup, NN)

    @pl.when(step == pl.num_programs(0) - 1)
    def _():
        rows = acc_g.shape[0] // 4
        spread(acc_g, rows, outs[:4])
        spread(acc_u, rows, outs[4:])


def first(h, by, gate, up, wd, start, width, load=None, step_us=1.0, tile=512, part=256):
    n, d = h.shape
    block = math.gcd(start, width)
    blocks = width // block
    rows = lambda: pl.BlockSpec((tile, d), lambda i: (i, 0))
    kept = [pl.BlockSpec((tile, block), lambda i, k=k: (i, start // block + k)) for k in range(blocks)]
    wds = [once((block, d), lambda i, k=k: (start // block + k, 0)) for k in range(blocks)]
    outs, done = call_with(
        load,
        step_us,
        functools.partial(first_body, part, blocks),
        f"first{start}",
        (n // tile,),
        [rows(), rows()] + kept * 2 + wds,
        spread_specs(d // 4, width, 8),
        spread_shapes(d // 4, width, 8),
        [pltpu.VMEM((d, width), F32)] * 2,
        6 * n * d * width,
        n * width * 8,
        (h, by, *[gate] * blocks, *[up] * blocks, *[wd] * blocks),
    )
    return outs[:4], outs[4:8], done


def tail_body(count, squares, load, *refs):
    n_in, n_out = len(load.in_specs), len(load.out_specs)
    others, refs = refs[:squares], refs[squares:]
    ins, refs = refs[:n_in], refs[n_in:]
    outs, factor_ref, refs = refs[:n_out], refs[n_out], refs[n_out + 1 :]
    scratch, (mine, got_core, both, got_x, send, recv) = refs[: len(load.scratch)], refs[len(load.scratch) :]
    place = Place()
    sums = load.sums(place, ins, outs, scratch)
    place.meet()
    for _, i, phase in timeline(load.sizes, load.kinds, 0, 0.0):
        sums[i].run(phase)
    total = sum(ref[...] for ref in others) + sum(one.square[...] for one in sums)
    mine[...] = total
    hop = remote(mine, got_core, send.at[0], recv.at[0], place.core)
    hop.start()
    hop.wait()
    both[...] = mine[...] + got_core[...]
    hop = remote(both, got_x, send.at[1], recv.at[1], place.over_x)
    hop.start()
    hop.wait()
    factor_ref[...] = jnp.minimum(1.0, 0.5 * lax.rsqrt((both[...] + got_x[...]) / count + 1e-30))


def tail(load, squares, count):
    whole = pl.BlockSpec((8, 128), lambda: (0, 0))
    outs = call(
        functools.partial(tail_body, count, len(squares), load),
        "tail",
        (),
        [whole] * len(squares) + load.in_specs,
        [pl.BlockSpec(one.block_shape, lambda: (0, 0)) for one in load.out_specs] + [whole],
        load.out_shape + [shape((8, 128), F32)],
        load.scratch + [pltpu.VMEM((8, 128), F32)] * 4 + [pltpu.SemaphoreType.DMA((2,))] * 2,
        1000,
        1000,
        load.id,
        SMALL,
    )(*squares, *load.args)
    return load.results(outs[:-1]), outs[-1]


def adamw(w, m, v, g):
    m = 0.9 * m + 0.1 * g
    v = 0.95 * v + 0.05 * g * g
    step = m * lax.rsqrt(v + 1e-8) + 0.1 * w
    return (w - 0.02 * step).astype(BF16), m, v


def update_body(edges, factor_ref, *refs):
    total = sum(len(edge) - 1 for per_layer in edges for edge in per_layer)
    grads, refs = refs[:total], refs[total:]
    states, news = refs[:9], refs[9:]
    turn = pl.program_id(0)
    factor = factor_ref[0, 0]
    k = 0
    for i, per_layer in enumerate(edges):
        for number, edge in enumerate(per_layer):
            for low, high in zip(edge, edge[1:]):

                @pl.when((turn >= low) & (turn < high))
                def _(ref=grads[k], i=i, number=number):
                    w, m, v = (states[3 * which + i][number] for which in range(3))
                    for which, one in enumerate(adamw(w.astype(F32), m, v, ref[...].astype(F32) * factor)):
                        news[3 * which + i][number] = one

                k += 1


def update(factor, pieces, states, turns=10):
    specs, edges, args = [pl.BlockSpec(memory_space=pltpu.SMEM)], [], [factor]
    state_specs = []
    for i, per_layer in enumerate(pieces):
        layers, rows, cols = states[i].shape
        tall = i == 2
        block = (rows // turns, cols) if tall else (rows, cols // turns)
        edges.append([])
        for parts in per_layer:
            edge = [0]
            for part in parts:
                low = edge[-1]
                edge.append(low + (part.shape[0] // block[0] if tall else part.shape[1] // block[1]))

                def index(turn, low=low, top=edge[-1] - low - 1, tall=tall):
                    at = jnp.clip(turn - low, 0, top)
                    return (at, 0) if tall else (0, at)

                specs.append(pl.BlockSpec(block, index))
                args.append(part)
            edges[-1].append(edge)
        state_specs.append(pl.BlockSpec((layers, *block), (lambda turn: (0, turn, 0)) if tall else (lambda turn: (0, 0, turn))))
    return call(
        functools.partial(update_body, edges),
        "update",
        (turns,),
        specs + state_specs * 3,
        state_specs * 3,
        [shape(one.shape, one.dtype) for one in states],
        [],
        1000000,
        1000000,
        limit=SMALL,
    )(*args, *states)


def solution(mesh):
    ns = mesh.shape["s"]

    def step(x, dy, *arrays):
        weights, m, v = (arrays[i : i + 3] for i in (0, 3, 6))
        h0, dy = x[0], dy[0]
        (gate, up, prod), (wd0, wg1, wu1) = project(h0, weights)
        h1, wd1 = down(h0, prod, wd0, weights[2])
        a = last(h1, dy, wg1, wu1, wd1, 0, 2)
        b = last(h1, dy, wg1, wu1, wd1, 1, 2, Load(1, [("all", a[2], None), ("all", a[3], None)]), 9.0)
        g1a, u1a = b[5]
        d1 = [a[4][0], b[4][0], a[4][1], b[4][1]]
        load = Load(2, [("all", b[2], None), ("all", b[3], None), ("x", d1, None)])
        by, (g1b, u1b, d1) = inward(h1, dy, [a[0], b[0]], [a[1], b[1]], wg1, wu1, load, 6.4)
        d0, (d1,) = outer(by, prod, Load(3, [("yz", [d1], None)]), 3.1)
        halves = lambda terms, cut, by=1: [("all", terms, (by, 0, cut)), ("all", terms, (by, cut, terms[0].shape[by] - cut))]
        c = first(h0, by, gate, up, wd0, 0, 1536, Load(4, halves(d0, 384, 0)), 7.2)
        d0 = c[2]
        load = Load(5, [one for pair in zip(halves(c[0], 768), halves(c[1], 768)) for one in pair])
        e = first(h0, by, gate, up, wd0, 1536, 1024, load, 4.8)
        g0a, u0a, g0b, u0b = e[2]
        done = [g1a, u1a, g1b, u1b, d1, *d0, *e[2]]
        count = ns * sum(w.size for w in weights)
        load = Load(6, [one for pair in zip(halves(e[0], 512), halves(e[1], 512)) for one in pair])
        (g0c, u0c, g0d, u0d), factor = tail(load, [one[1] for one in done], count)
        parts = lambda *ones: [one[0] for one in ones]
        pieces = [
            [parts(g0a, g0b, g0c, g0d), parts(g1a, g1b)],
            [parts(u0a, u0b, u0c, u0d), parts(u1a, u1b)],
            [parts(*d0), parts(d1)],
        ]
        return tuple(update(factor, pieces, [*weights, *m, *v]))

    states, cut = P(("rep", "r", "s"), None, None), P(None, "s", None)
    return jax.shard_map(
        step,
        mesh=mesh,
        in_specs=(states, states) + (cut,) * 9,
        out_specs=(P("rep", "s", None),) * 9,
        check_vma=False,
    )
```

```python
import functools
import math

import jax
import jax.numpy as jnp
from jax import lax
from jax.experimental import pallas as pl
from jax.experimental.pallas import tpu as pltpu
from jax.sharding import PartitionSpec as P

NAMES = ("w_gate", "w_up", "w_down")
F32, BF16 = jnp.float32, jnp.bfloat16
MESH = pl.DeviceIdType.MESH
VMEM_LIMIT = 60 * 1024 * 1024
SMALL = VMEM_LIMIT


def dot(a, b, dims):
    return lax.dot_general(a, b, (dims, ((), ())), preferred_element_type=F32)


NN, NT, TN = ((1,), (0,)), ((1,), (1,)), ((0,), (0,))


def normed(h):
    wide = h.astype(F32)
    scale = lax.rsqrt(jnp.mean(wide * wide, -1, keepdims=True) + 1e-6)
    return (wide * scale).astype(BF16)


def call(body, name, grid, in_specs, out_specs, out_shape, scratch, flops, moved, sends=None, limit=VMEM_LIMIT):
    remote = {} if sends is None else {"collective_id": sends, "has_side_effects": True}
    return pl.pallas_call(
        body,
        grid=grid,
        in_specs=in_specs,
        out_specs=out_specs,
        out_shape=out_shape,
        scratch_shapes=scratch,
        name=name,
        compiler_params=pltpu.CompilerParams(dimension_semantics=("arbitrary",) * len(grid), vmem_limit_bytes=limit, **remote),
        cost_estimate=pl.CostEstimate(flops=flops, bytes_accessed=moved, transcendentals=0),
    )


def once(shape, index):
    return pl.BlockSpec(shape, index, pipeline_mode=pl.Buffered(1))


def shape(dims, dtype):
    return jax.ShapeDtypeStruct(dims, dtype)


class Place:
    def __init__(self):
        s, r = lax.axis_index("s"), lax.axis_index("r")
        self.s, self.r = s, r
        self.x, self.c = s // 2, s % 2
        self.s_core, self.s_x = s + 1 - 2 * self.c, (s + 2) % 4
        self.s_both = (self.s_core + 2) % 4
        self.r_y, self.r_z = (r + 2) % 4, r + 1 - 2 * (r % 2)
        self.r_yz = (self.r_z + 2) % 4
        self.core, self.over_x = {"s": self.s_core}, {"s": self.s_x}
        self.over_y, self.over_z = {"r": self.r_y}, {"r": self.r_z}

    def meet(self):
        barrier = pltpu.get_barrier_semaphore()
        for one in (self.core, self.over_x, self.over_y, self.over_z):
            pl.semaphore_signal(barrier, inc=1, device_id=one, device_id_type=MESH)
        pl.semaphore_wait(barrier, 4)


def remote(src, dst, send, recv, device):
    return pltpu.make_async_remote_copy(
        src_ref=src, dst_ref=dst, send_sem=send, recv_sem=recv, device_id=device, device_id_type=MESH
    )


class Sum:
    FIRST = {"all": 0, "x": 0, "yz": 2}
    LAST = {"all": 4, "x": 2, "yz": 4}

    def __init__(self, place, kind, refs, outs, scratch):
        self.place, self.kind, self.refs, self.out = place, kind, refs, outs[0]
        self.square = outs[1] if kind != "x" else None
        self.local, self.send, self.recv = scratch[-3:]
        scratch = scratch[:-3]
        if kind != "yz":
            self.kept, self.got, self.far, self.got_x = scratch[:4]
            scratch = scratch[4:]
        if kind != "x":
            self.near, self.got_1, self.pair, self.got_2 = scratch
        half = self.out.shape[0] // 2
        self.top, self.low = pl.ds(0, half), pl.ds(half, half)

    @staticmethod
    def scratch(kind, rows, cols):
        one = lambda *lead: pltpu.VMEM((*lead, rows, cols), BF16)
        to_x = [one(2), one(2), one(), one()] if kind != "yz" else []
        to_yz = [one()] * 4 if kind != "x" else []
        return to_x + to_yz + [pltpu.SemaphoreType.DMA((k,)) for k in (2, 7, 7)]

    def copies(self, phase):
        p, over = self.place, lambda i, src, dst, to: remote(src, dst, self.send.at[i], self.recv.at[i], to)
        if phase == 0:
            return [over(i, self.refs[2 + i], self.got.at[i], p.core) for i in range(2)]
        if phase == 1:
            return [over(2, self.far, self.got_x, p.over_x)]
        if phase == 2:
            return [
                over(3, self.near.at[self.top], self.got_1.at[self.top], p.over_y),
                over(4, self.near.at[self.low], self.got_1.at[self.low], p.over_z),
            ]
        return [
            over(5, self.pair.at[self.top], self.got_2.at[self.top], p.over_z),
            over(6, self.pair.at[self.low], self.got_2.at[self.low], p.over_y),
        ]

    def locals(self):
        if self.kind == "yz":
            return [pltpu.make_async_copy(self.refs[0], self.near, self.local.at[0])]
        return [pltpu.make_async_copy(self.refs[i], self.kept.at[i], self.local.at[i]) for i in range(2)]

    def run(self, phase):
        x = self.place.x
        wide = lambda ref: ref.astype(F32)
        if phase == 0:
            for one in self.locals() + self.copies(0):
                one.start()
            return
        if phase == 2 and self.kind == "yz":
            for one in self.locals():
                one.start()
                one.wait()
        else:
            for one in self.copies(phase - 1):
                one.wait()
        if phase == 1:
            for one in self.locals():
                one.wait()
            self.far[...] = (wide(self.kept[1 - x]) + wide(self.got[1 - x])).astype(BF16)
        elif phase == 2 and self.kind != "yz":
            into = self.out if self.kind == "x" else self.near
            into[...] = (wide(self.kept[x]) + wide(self.got[x]) + wide(self.got_x[...])).astype(BF16)
        elif phase == 3:
            self.pair[...] = (wide(self.near[...]) + wide(self.got_1[...])).astype(BF16)
        elif phase == 4:
            total = (wide(self.pair[...]) + wide(self.got_2[...])).astype(BF16)
            self.out[...] = total
            self.square[...] = jnp.full(self.square.shape, jnp.sum(wide(total) * wide(total)), F32)
        if phase < Sum.LAST[self.kind]:
            for one in self.copies(phase):
                one.start()


def timeline(sizes, kinds, steps, step_us):
    rate = {"core": 4e5, "x": 4.6e4, "y": 4.6e4, "z": 4.6e4}
    free = dict.fromkeys(rate, 0.0)
    parts = {0: (("core", 2.0),), 1: (("x", 1.0),), 2: (("y", 0.5), ("z", 0.5)), 3: (("y", 0.5), ("z", 0.5))}
    phase = [Sum.FIRST[kind] for kind in kinds]
    ready, order, now, k = [0.0] * len(sizes), [], 0.0, 0
    while any(p <= Sum.LAST[kind] for p, kind in zip(phase, kinds)):
        waiting = [i for i, kind in enumerate(kinds) if phase[i] <= Sum.LAST[kind]]
        able = [i for i in waiting if ready[i] <= now]
        if not able and k < steps:
            k += 1
            now = max(now, k * step_us)
            continue
        i = min(able or waiting, key=lambda j: (ready[j], -phase[j], j))
        now = max(now, ready[i])
        order.append((k, i, phase[i]))
        ends = [now]
        for link, share in parts.get(phase[i], ()):
            free[link] = max(free[link], now) + share * sizes[i][0] * sizes[i][1] * 2 / rate[link]
            ends.append(free[link] + 2.0)
        ready[i] = max(ends)
        phase[i] += 1
    return order


class Load:
    def __init__(self, id, jobs):
        self.id = id
        self.kinds = [kind for kind, _, _ in jobs]
        self.parts = [part for _, _, part in jobs]
        self.sizes = [
            tuple(part[2] if part and part[0] == i else size for i, size in enumerate(terms[0].shape)) for _, terms, part in jobs
        ]
        self.counts = [len(terms) for _, terms, _ in jobs]
        self.args = [ref for _, terms, _ in jobs for ref in terms]
        self.in_specs = [pl.BlockSpec(memory_space=pl.ANY)] * len(self.args)
        here = lambda *_: (0, 0)
        results = [
            each for size, kind in zip(self.sizes, self.kinds) for each in [(size, BF16)] + ([] if kind == "x" else [((8, 128), F32)])
        ]
        self.out_specs = [once(size, here) for size, _ in results]
        self.out_shape = [shape(size, dtype) for size, dtype in results]
        self.scratch = [ref for size, kind in zip(self.sizes, self.kinds) for ref in Sum.scratch(kind, *size)]

    def sums(self, place, ins, outs, scratch):
        made = []
        for kind, part, size, count in zip(self.kinds, self.parts, self.sizes, self.counts):
            terms, ins = ins[:count], ins[count:]
            if part is not None:
                at = pl.ds(*part[1:])
                terms = [ref.at[at] if part[0] == 0 else ref.at[:, at] for ref in terms]
            n = 1 if kind == "x" else 2
            m = len(Sum.scratch(kind, *size))
            made.append(Sum(place, kind, terms, outs[:n], scratch[:m]))
            outs, scratch = outs[n:], scratch[m:]
        return made

    def results(self, outs):
        made = []
        for kind in self.kinds:
            n = 1 if kind == "x" else 2
            made.append(outs[0] if n == 1 else (outs[0], outs[1]))
            outs = outs[n:]
        return made


def carried(body, load, own_in, own_out, steps, step_us, hooks):
    order = timeline(load.sizes, load.kinds, steps * hooks, step_us / hooks)

    def both(*refs):
        n_in, n_out, n_scratch = len(load.in_specs), len(load.out_specs), len(load.scratch)
        ins, refs = refs[:own_in], refs[own_in:]
        more_in, refs = refs[:n_in], refs[n_in:]
        outs, refs = refs[:own_out], refs[own_out:]
        more_out, refs = refs[:n_out], refs[n_out:]
        scratch, more_scratch = refs[: len(refs) - n_scratch], refs[len(refs) - n_scratch :]
        place = Place()
        step = pl.program_id(0)
        sums = load.sums(place, more_in, more_out, more_scratch)

        def act(at):
            todo = [(i, phase) for when, i, phase in order if when == at]
            if todo:

                @pl.when(step == min(at // hooks, steps - 1))
                def _():
                    if at == 0:
                        place.meet()
                    for i, phase in todo:
                        sums[i].run(phase)

        def pause(now):
            for at in range(now, steps * hooks, hooks):
                act(at)

        pause(0)
        body(*ins, *outs, *scratch, **({"pause": pause} if hooks > 1 else {}))
        act(steps * hooks)

    return both


def call_with(load, step_us, hooks, body, name, grid, in_specs, out_specs, out_shape, scratch, flops, moved, args):
    if load is None:
        outs = call(body, name, grid, in_specs, out_specs, out_shape, scratch, flops, moved)(*args)
        return list(outs), []
    outs = call(
        carried(body, load, len(in_specs), len(out_specs), grid[0], step_us, hooks),
        name,
        grid,
        in_specs + load.in_specs,
        out_specs + load.out_specs,
        out_shape + load.out_shape,
        scratch + load.scratch,
        flops,
        moved,
        load.id,
    )(*args, *load.args)
    return list(outs[: len(out_specs)]), load.results(outs[len(out_specs) :])


def spread(acc, rows, refs):
    c = lax.axis_index("s") % 2
    for i, ref in enumerate(refs):
        at = (i % 2) * 2 + (c if i < 2 else 1 - c)
        ref[...] = acc[pl.ds(pl.multiple_of(at * rows, rows), rows), :].astype(BF16)


def spread_shapes(rows, cols, count=4):
    return [shape((rows, cols), BF16)] * count


def spread_specs(rows, cols, count=4):
    return [once((rows, cols), lambda *_: (0, 0))] * count


def clear(step, *refs):
    @pl.when(step == 0)
    def _():
        for ref in refs:
            ref[...] = jnp.zeros_like(ref)


class Fetch:
    COPIES = 9

    def __init__(self, place, own, full, columns, send, recv, local, stage=None):
        self.place, self.own, self.full, self.columns = place, own, full, columns
        self.send, self.recv, self.local, self.stage = send, recv, local, stage

    def part(self, block, quarter=None):
        rows = self.own.shape[0]
        if self.columns is None:
            if quarter is None:
                return self.full.at[pl.ds(pl.multiple_of(block * rows, rows), rows)]
            return self.full.at[pl.ds(pl.multiple_of(block * rows + quarter * (rows // 4), rows // 4), rows // 4)]
        start, width = self.columns
        across = pl.ds(start, width) if quarter is None else pl.ds(pl.multiple_of(start + quarter * (width // 4), 128), width // 4)
        return self.full.at[pl.ds(pl.multiple_of(block * rows, rows), rows), across]

    def mine(self, quarter=None):
        rows = self.own.shape[0]
        if self.columns is None:
            return self.own if quarter is None else self.own.at[pl.ds(pl.multiple_of(quarter * (rows // 4), rows // 4), rows // 4)]
        start, width = self.columns
        across = pl.ds(start, width) if quarter is None else pl.ds(pl.multiple_of(start + quarter * (width // 4), 128), width // 4)
        return self.own.at[:, across]

    def copy(self, i):
        p = self.place
        over = lambda src, dst, to: remote(src, dst, self.send.at[i], self.recv.at[i], to)
        if i == 0:
            return over(self.mine(), self.part(p.s), p.core)
        if i in (1, 2):
            q = p.r if i == 1 else p.r_yz
            return over(self.mine(q), self.part(p.s, q), p.over_x)
        if i in (3, 4):
            return over(self.part(p.s_x, p.r), self.part(p.s_x, p.r), p.over_y if i == 3 else p.over_z)
        q = (p.r, p.r_yz, p.r_y, p.r_z)[i - 5]
        return over(self.part(p.s_x, q), self.part(p.s_x, q), p.core)

    def received(self, i):
        p = self.place
        if i == 0:
            return self.part(p.s_core)
        block, q = [(p.s_x, p.r), (p.s_x, p.r_yz), (p.s_x, p.r_y), (p.s_x, p.r_z)][i - 1] if i < 5 else (p.s_both, (p.r, p.r_yz, p.r_y, p.r_z)[i - 5])
        return self.part(block, q)

    def start(self, *which):
        for i in which:
            self.copy(i).start()

    def arrived(self, i):
        here = self.received(i)
        remote(here, here, self.send.at[i], self.recv.at[i], self.place.core).wait_recv()

    def begin(self):
        self.start(1, 0)
        into = self.stage if self.stage is not None else self.part(self.place.s)
        pltpu.make_async_copy(self.mine(), into, self.local.at[0]).start()

    def begin_last(self):
        self.start(2)

    def relay(self):
        self.arrived(1)
        self.start(3, 4, 5)
        if self.stage is not None:
            pltpu.make_async_copy(self.mine(), self.stage, self.local.at[0]).wait()
            pltpu.make_async_copy(self.stage, self.part(self.place.s), self.local.at[1]).start()

    def hand_over(self):
        self.arrived(3)
        self.start(7)
        self.arrived(4)
        self.start(8)

    def hand_last(self):
        self.arrived(2)
        self.start(6)

    def finish(self):
        if self.stage is not None:
            pltpu.make_async_copy(self.stage, self.part(self.place.s), self.local.at[1]).wait()
        else:
            pltpu.make_async_copy(self.mine(), self.part(self.place.s), self.local.at[0]).wait()
        for i in (0, 5, 6, 7, 8):
            self.arrived(i)
        for i in range(self.COPIES):
            self.copy(i).wait_send()


RUN = 512


def project_body(h_ref, *refs):
    g, u, d, refs = *refs[:3], refs[3:]
    gate_ref, up_ref, prod_ref = refs[:3]
    full, refs = refs[3:5], refs[5:]
    a_all, wg, wu, stage_d0, stage_g1, send, recv, local = refs
    run, tile = pl.program_id(0), pl.program_id(1)
    step = run * pl.num_programs(1) + tile
    place = Place()
    ff = wg.shape[1]
    plan = [(own.at[0], whole, across, None) for across in ((0, 512), (512, 1024), (1536, 1024)) for own, whole in ((g, wg), (u, wu))]
    plan += [(d.at[0], full[0], None, stage_d0), (g.at[1], full[1], (0, ff), stage_g1)]
    fetches = [
        Fetch(place, mine, whole, columns, send.at[i], recv.at[i], local.at[i], stage) for i, (mine, whole, columns, stage) in enumerate(plan)
    ]

    def act(when, *moves):
        @pl.when(step == when)
        def _():
            for numbers, *what in moves:
                for each in what:
                    for number in numbers:
                        getattr(fetches[number], each)()

    @pl.when(step == 0)
    def _():
        place.meet()

    a, b, c, d0, g1 = (0, 1), (2, 3), (4, 5), (6,), (7,)
    act(0, (a, "begin", "begin_last"), (b, "begin", "begin_last"), (a, "relay", "hand_over", "hand_last", "finish"))
    act(1, (b, "relay"), (c, "begin", "begin_last"))
    act(4, (b, "hand_over", "hand_last", "finish"), (d0, "begin", "begin_last"))
    act(6, (c, "relay"))
    act(8, (g1, "begin", "begin_last"))
    act(9, (c, "hand_over", "hand_last"))
    act(11, (c, "finish"), (d0, "relay"))
    act(14, (d0, "hand_over", "hand_last"))
    act(16, (g1, "relay"))
    rows = h_ref.shape[0]
    mine = pl.ds(pl.multiple_of(tile * rows, rows), rows)

    @pl.when(run == 0)
    def _():
        a_all[mine, :] = normed(h_ref[...])

    a = a_all[mine, :]
    part = RUN // 2
    front = lambda i: [
        dot(a, w[:, pl.ds(pl.multiple_of(run * RUN + i * part, part), part)], NN) for w in (wg, wu)
    ]
    ahead = front(0)
    for i in range(2):
        gate, up = ahead
        if i == 0:
            ahead = front(1)
        at = slice(i * part, (i + 1) * part)
        gate_ref[:, at] = gate
        up_ref[:, at] = up
        prod_ref[:, at] = (gate * jax.nn.sigmoid(gate) * up).astype(BF16)
    act(19, (g1, "hand_over", "hand_last"), (d0, "finish"), (g1, "finish"))


def project(h, weights, tile=1024):
    n, d = h.shape
    ff = weights[0].shape[2]
    sizes = [one.shape[1:] for one in (weights[2], weights[0])]
    rows = pl.BlockSpec((tile, RUN), lambda i, j: (j, i))
    hbm = pl.BlockSpec(memory_space=pl.ANY)
    outs = call(
        project_body,
        "project",
        (ff // RUN, n // tile),
        [pl.BlockSpec((tile, d), lambda i, j: (jnp.where(i == 0, j, n // tile - 1), 0))] + [hbm] * 3,
        [rows] * 3 + [hbm] * 2,
        [shape((n, ff), F32), shape((n, ff), F32), shape((n, ff), BF16)]
        + [shape((high * 4, cols), BF16) for high, cols in sizes],
        [pltpu.VMEM((n, d), BF16), pltpu.VMEM((d, ff), BF16), pltpu.VMEM((d, ff), BF16)]
        + [pltpu.VMEM(size, BF16) for size in sizes]
        + [pltpu.SemaphoreType.DMA((8, 9)), pltpu.SemaphoreType.DMA((8, 9)), pltpu.SemaphoreType.DMA((8, 2))],
        4 * n * d * ff,
        n * ff * 10,
        0,
    )(h, *weights)
    return outs[:3], outs[3:]


def down_body(h_ref, prod_ref, wd_ref, u_ref, d_ref, out_ref, full_u, full_d, stage_u, stage_d, send, recv, local):
    step = pl.program_id(0)
    place = Place()
    plan = [(u_ref.at[1], full_u, (0, u_ref.shape[2]), stage_u), (d_ref.at[1], full_d, None, stage_d)]
    fetches = [
        Fetch(place, mine, whole, columns, send.at[i], recv.at[i], local.at[i], stage) for i, (mine, whole, columns, stage) in enumerate(plan)
    ]

    def act(when, *moves):
        @pl.when(step == when)
        def _():
            if when == 0:
                place.meet()
            for numbers, *what in moves:
                for each in what:
                    for number in numbers:
                        getattr(fetches[number], each)()

    act(0, ((0, 1), "begin", "begin_last"))
    act(3, ((0,), "relay"))
    act(5, ((1,), "relay"))
    act(6, ((0,), "hand_over"))
    out_ref[...] = h_ref[...] + dot(prod_ref[...], wd_ref[...], NN).astype(BF16)
    act(pl.num_programs(0) - 1, ((0,), "hand_last"), ((1,), "hand_over", "hand_last"), ((0, 1), "finish"))


def down(h, prod, wd, w_up, w_down, tile=512):
    n, d = h.shape
    ff = wd.shape[0]
    rows = lambda width: pl.BlockSpec((tile, width), lambda i: (i, 0))
    hbm = pl.BlockSpec(memory_space=pl.ANY)
    return call(
        down_body,
        "down",
        (n // tile,),
        [rows(d), rows(ff), once((ff, d), lambda i: (0, 0)), hbm, hbm],
        [rows(d), hbm, hbm],
        [shape((n, d), BF16), shape((d, ff), BF16), shape((ff, d), BF16)],
        [pltpu.VMEM(one.shape[1:], BF16) for one in (w_up, w_down)]
        + [pltpu.SemaphoreType.DMA((2, 9)), pltpu.SemaphoreType.DMA((2, 9)), pltpu.SemaphoreType.DMA((2, 2))],
        2 * n * d * ff,
        n * ff * 2,
        7,
    )(h, prod, wd, w_up, w_down)


def slopes(gate, up, dprod):
    s = jax.nn.sigmoid(gate)
    silu = gate * s
    return silu, (dprod * silu).astype(BF16), (dprod * up * (s + silu * (1 - s))).astype(BF16)


def last_body(part, h_ref, dy_ref, wg_ref, wu_ref, wd_ref, dgate_ref, dup_ref, *rest):
    outs, (acc_g, acc_u, acc_d) = rest[:10], rest[10:]
    step = pl.program_id(0)
    clear(step, acc_g, acc_u, acc_d)
    a = normed(h_ref[...])
    dy = dy_ref[...]
    a_t, dy_t = a.T, dy.T
    parts = [slice(i, i + part) for i in range(0, wg_ref.shape[1], part)]
    front = lambda at: (dot(a, wg_ref[:, at], NN), dot(a, wu_ref[:, at], NN), dot(dy, wd_ref[at, :], NT))
    ahead = front(parts[0])
    for i, at in enumerate(parts):
        gate, up, dprod = ahead
        if i + 1 < len(parts):
            ahead = front(parts[i + 1])
        silu, dup, dgate = slopes(gate, up, dprod.astype(BF16).astype(F32))
        dgate_ref[:, at] = dgate
        dup_ref[:, at] = dup
        acc_g[:, at] += dot(a_t, dgate, NN)
        acc_u[:, at] += dot(a_t, dup, NN)
        acc_d[:, at] += dot(dy_t, (silu * up).astype(BF16), NN)

    @pl.when(step == pl.num_programs(0) - 1)
    def _():
        rows = acc_g.shape[0] // 4
        spread(acc_g, rows, outs[:4])
        spread(acc_u, rows, outs[4:8])
        c = lax.axis_index("s") % 2
        rows = acc_d.shape[1] // 2
        for core, ref in ((c, outs[8]), (1 - c, outs[9])):
            ref[...] = acc_d[:, pl.ds(pl.multiple_of(core * rows, rows), rows)].T.astype(BF16)


def last(h, dy, wg, wu, wd, run, runs, load=None, step_us=1.0, tile=512, part=256):
    n, d = h.shape
    ff = wg.shape[1] // runs
    rows = lambda width: pl.BlockSpec((tile, width), lambda i: (i, 0))
    columns = lambda: once((d, ff), lambda i: (0, run))
    outs, done = call_with(
        load,
        step_us,
        1,
        functools.partial(last_body, part),
        f"last{run}",
        (n // tile,),
        [rows(d), rows(d), columns(), columns(), once((ff, d), lambda i: (run, 0))],
        [rows(ff), rows(ff)] + spread_specs(d // 4, ff, 8) + spread_specs(ff // 2, d, 2),
        [shape((n, ff), BF16)] * 2 + spread_shapes(d // 4, ff, 8) + spread_shapes(ff // 2, d, 2),
        [pltpu.VMEM((d, ff), F32)] * 3,
        12 * n * d * ff,
        n * ff * 4,
        (h, dy, wg, wu, wd),
    )
    return outs[0], outs[1], outs[2:6], outs[6:10], outs[10:12], done


def inward_body(runs, h_ref, by_ref, *rest, pause):
    dgates, dups, (wg_ref, wu_ref, out_ref) = rest[:runs], rest[runs : 2 * runs], rest[2 * runs :]
    ff = dgates[0].shape[1]
    total = lambda parts, w: sum(dot(p[...], w[:, i * ff : (i + 1) * ff], NT) for i, p in enumerate(parts)).astype(BF16)
    da = total(dgates, wg_ref)
    pause(1)
    da = (da + total(dups, wu_ref)).astype(F32)
    wide = h_ref[...].astype(F32)
    scale = lax.rsqrt(jnp.mean(wide * wide, -1, keepdims=True) + 1e-6)
    along = jnp.mean(da * wide, -1, keepdims=True)
    dh = da * scale - wide * (scale * scale * scale * along)
    out_ref[...] = by_ref[...] + dh.astype(BF16)


def inward(h, by, dgates, dups, wg, wu, load=None, step_us=1.0, tile=512):
    n, d = h.shape
    ff = wg.shape[1]
    runs = len(dgates)
    rows = lambda width: pl.BlockSpec((tile, width), lambda i: (i, 0))
    outs, done = call_with(
        load,
        step_us,
        2,
        functools.partial(inward_body, runs),
        "inward",
        (n // tile,),
        [rows(d), rows(d)] + [rows(ff // runs)] * (2 * runs) + [once((d, ff), lambda i: (0, 0))] * 2,
        [rows(d)],
        [shape((n, d), BF16)],
        [],
        4 * n * d * ff,
        n * ff * 4,
        (h, by, *dgates, *dups, wg, wu),
    )
    return outs[0], done


def outer_body(by_ref, prod_ref, *rest):
    outs, acc = rest[:4], rest[4]
    step = pl.program_id(0)
    clear(step, acc)
    acc[...] += dot(by_ref[...].T, prod_ref[...], NN)

    @pl.when(step == pl.num_programs(0) - 1)
    def _():
        c = lax.axis_index("s") % 2
        rows = acc.shape[1] // 4
        for i, ref in enumerate(outs):
            block = (i % 2) * 2 + (c if i < 2 else 1 - c)
            ref[...] = acc[:, pl.ds(pl.multiple_of(block * rows, rows), rows)].T.astype(BF16)


def outer(by, prod, load=None, step_us=1.0, tile=512):
    n, d = by.shape
    ff = prod.shape[1]
    rows = lambda width: pl.BlockSpec((tile, width), lambda i: (i, 0))
    return call_with(
        load,
        step_us,
        1,
        outer_body,
        "outer",
        (n // tile,),
        [rows(d), rows(ff)],
        spread_specs(ff // 4, d),
        spread_shapes(ff // 4, d),
        [pltpu.VMEM((d, ff), F32)],
        2 * n * d * ff,
        n * ff * 2,
        (by, prod),
    )


def first_body(part, blocks, h_ref, by_ref, *rest, pause):
    gates, ups, wds, rest = rest[:blocks], rest[blocks : 2 * blocks], rest[2 * blocks : 3 * blocks], rest[3 * blocks :]
    outs, (acc_g, acc_u) = rest[:8], rest[8:]
    step = pl.program_id(0)
    clear(step, acc_g, acc_u)
    a_t = normed(h_ref[...]).T
    by = by_ref[...]
    width = wds[0].shape[0]
    parts = [(k, slice(i, i + part)) for k in range(blocks) for i in range(0, width, part)]
    front = lambda k, at: dot(by, wds[k][at, :], NT)
    ahead = front(*parts[0])
    for i, (k, at) in enumerate(parts):
        if i == len(parts) // 2:
            pause(1)
        dprod = ahead.astype(BF16).astype(F32)
        if i + 1 < len(parts):
            ahead = front(*parts[i + 1])
        _, dup, dgate = slopes(gates[k][:, at], ups[k][:, at], dprod)
        to = slice(i * part, (i + 1) * part)
        acc_g[:, to] += dot(a_t, dgate, NN)
        acc_u[:, to] += dot(a_t, dup, NN)

    @pl.when(step == pl.num_programs(0) - 1)
    def _():
        rows = acc_g.shape[0] // 4
        spread(acc_g, rows, outs[:4])
        spread(acc_u, rows, outs[4:])


def first(h, by, gate, up, wd, start, width, load=None, step_us=1.0, tile=512, part=256):
    n, d = h.shape
    block = math.gcd(start, width)
    blocks = width // block
    rows = lambda: pl.BlockSpec((tile, d), lambda i: (i, 0))
    kept = [pl.BlockSpec((tile, block), lambda i, k=k: (i, start // block + k)) for k in range(blocks)]
    wds = [once((block, d), lambda i, k=k: (start // block + k, 0)) for k in range(blocks)]
    outs, done = call_with(
        load,
        step_us,
        2,
        functools.partial(first_body, part, blocks),
        f"first{start}",
        (n // tile,),
        [rows(), rows()] + kept * 2 + wds,
        spread_specs(d // 4, width, 8),
        spread_shapes(d // 4, width, 8),
        [pltpu.VMEM((d, width), F32)] * 2,
        6 * n * d * width,
        n * width * 8,
        (h, by, *[gate] * blocks, *[up] * blocks, *[wd] * blocks),
    )
    return outs[:4], outs[4:8], done


def tail_body(count, squares, load, *refs):
    n_in, n_out = len(load.in_specs), len(load.out_specs)
    others, refs = refs[:squares], refs[squares:]
    ins, refs = refs[:n_in], refs[n_in:]
    outs, factor_ref, refs = refs[:n_out], refs[n_out], refs[n_out + 1 :]
    scratch, (mine, got_core, both, got_x, send, recv) = refs[: len(load.scratch)], refs[len(load.scratch) :]
    place = Place()
    sums = load.sums(place, ins, outs, scratch)
    place.meet()
    for _, i, phase in timeline(load.sizes, load.kinds, 0, 0.0):
        sums[i].run(phase)
    total = sum(ref[...] for ref in others) + sum(one.square[...] for one in sums)
    mine[...] = total
    hop = remote(mine, got_core, send.at[0], recv.at[0], place.core)
    hop.start()
    hop.wait()
    both[...] = mine[...] + got_core[...]
    hop = remote(both, got_x, send.at[1], recv.at[1], place.over_x)
    hop.start()
    hop.wait()
    factor_ref[...] = jnp.minimum(1.0, 0.5 * lax.rsqrt((both[...] + got_x[...]) / count + 1e-30))


def tail(load, squares, count):
    whole = pl.BlockSpec((8, 128), lambda: (0, 0))
    outs = call(
        functools.partial(tail_body, count, len(squares), load),
        "tail",
        (),
        [whole] * len(squares) + load.in_specs,
        [pl.BlockSpec(one.block_shape, lambda: (0, 0)) for one in load.out_specs] + [whole],
        load.out_shape + [shape((8, 128), F32)],
        load.scratch + [pltpu.VMEM((8, 128), F32)] * 4 + [pltpu.SemaphoreType.DMA((2,))] * 2,
        1000,
        1000,
        load.id,
        SMALL,
    )(*squares, *load.args)
    return load.results(outs[:-1]), outs[-1]


def adamw(w, m, v, g):
    m = 0.9 * m + 0.1 * g
    v = 0.95 * v + 0.05 * g * g
    step = m * lax.rsqrt(v + 1e-8) + 0.1 * w
    return (w - 0.02 * step).astype(BF16), m, v


def update_body(edges, factor_ref, *refs):
    total = sum(len(edge) - 1 for per_layer in edges for edge in per_layer)
    grads, refs = refs[:total], refs[total:]
    states, news = refs[:9], refs[9:]
    turn = pl.program_id(0)
    factor = factor_ref[0, 0]
    k = 0
    for i, per_layer in enumerate(edges):
        for number, edge in enumerate(per_layer):
            for low, high in zip(edge, edge[1:]):

                @pl.when((turn >= low) & (turn < high))
                def _(ref=grads[k], i=i, number=number):
                    w, m, v = (states[3 * which + i][number] for which in range(3))
                    for which, one in enumerate(adamw(w.astype(F32), m, v, ref[...].astype(F32) * factor)):
                        news[3 * which + i][number] = one

                k += 1


def update(factor, pieces, states, turns=10):
    specs, edges, args = [pl.BlockSpec(memory_space=pltpu.SMEM)], [], [factor]
    state_specs = []
    for i, per_layer in enumerate(pieces):
        layers, rows, cols = states[i].shape
        tall = i == 2
        block = (rows // turns, cols) if tall else (rows, cols // turns)
        edges.append([])
        for parts in per_layer:
            edge = [0]
            for part in parts:
                low = edge[-1]
                edge.append(low + (part.shape[0] // block[0] if tall else part.shape[1] // block[1]))

                def index(turn, low=low, top=edge[-1] - low - 1, tall=tall):
                    at = jnp.clip(turn - low, 0, top)
                    return (at, 0) if tall else (0, at)

                specs.append(pl.BlockSpec(block, index))
                args.append(part)
            edges[-1].append(edge)
        state_specs.append(pl.BlockSpec((layers, *block), (lambda turn: (0, turn, 0)) if tall else (lambda turn: (0, 0, turn))))
    return call(
        functools.partial(update_body, edges),
        "update",
        (turns,),
        specs + state_specs * 3,
        state_specs * 3,
        [shape(one.shape, one.dtype) for one in states],
        [],
        1000000,
        1000000,
        limit=SMALL,
    )(*args, *states)


def solution(mesh):
    ns = mesh.shape["s"]

    def step(x, dy, *arrays):
        weights, m, v = (arrays[i : i + 3] for i in (0, 3, 6))
        h0, dy = x[0], dy[0]
        (gate, up, prod), (wd0, wg1) = project(h0, weights)
        h1, wu1, wd1 = down(h0, prod, wd0, weights[1], weights[2])
        a = last(h1, dy, wg1, wu1, wd1, 0, 2)
        b = last(h1, dy, wg1, wu1, wd1, 1, 2, Load(1, [("all", a[2], None), ("all", a[3], None)]), 9.0)
        g1a, u1a = b[5]
        d1 = [a[4][0], b[4][0], a[4][1], b[4][1]]
        high, low = (0, 0, 384), (0, 384, 256)
        load = Load(2, [("all", b[2], None), ("all", b[3], None), ("x", d1, high)])
        by, (g1b, u1b, d1a) = inward(h1, dy, [a[0], b[0]], [a[1], b[1]], wg1, wu1, load, 6.2)
        d0, (d1a, d1b) = outer(by, prod, Load(3, [("yz", [d1a], None), ("x", d1, low)]), 3.1)
        load = Load(4, [("all", d0, high), ("x", d0, low), ("yz", [d1b], None)])
        c = first(h0, by, gate, up, wd0, 0, 1536, load, 5.6)
        d0a, d0b, d1b = c[2]
        left, right = (1, 0, 768), (1, 768, 768)
        load = Load(5, [("all", c[0], left), ("all", c[1], left), ("all", c[0], right), ("x", c[1], right), ("yz", [d0b], None)])
        e = first(h0, by, gate, up, wd0, 1536, 1024, load, 4.0)
        g0a, u0a, g0b, u0b, d0b = e[2]
        done = [g1a, u1a, g1b, u1b, d1a, d1b, d0a, d0b, g0a, u0a, g0b]
        count = ns * sum(w.size for w in weights)
        left, right = (1, 0, 512), (1, 512, 512)
        load = Load(6, [("all", e[0], left), ("all", e[1], left), ("all", e[0], right), ("all", e[1], right), ("yz", [u0b], None)])
        (g0c, u0c, g0d, u0d, u0b), factor = tail(load, [one[1] for one in done], count)
        parts = lambda *ones: [one[0] for one in ones]
        pieces = [
            [parts(g0a, g0b, g0c, g0d), parts(g1a, g1b)],
            [parts(u0a, u0b, u0c, u0d), parts(u1a, u1b)],
            [parts(d0a, d0b), parts(d1a, d1b)],
        ]
        return tuple(update(factor, pieces, [*weights, *m, *v]))

    states, cut = P(("rep", "r", "s"), None, None), P(None, "s", None)
    return jax.shard_map(
        step,
        mesh=mesh,
        in_specs=(states, states) + (cut,) * 9,
        out_specs=(P("rep", "s", None),) * 9,
        check_vma=False,
    )
```

```python
import functools

import jax
import jax.numpy as jnp
from jax import lax
from jax.experimental import pallas as pl
from jax.experimental.pallas import tpu as pltpu
from jax.sharding import PartitionSpec as P

NAMES = ("w_gate", "w_up", "w_down")
F32, BF16 = jnp.float32, jnp.bfloat16
MESH = pl.DeviceIdType.MESH
VMEM_LIMIT = 60 * 1024 * 1024
SMALL = VMEM_LIMIT
WHOLE = 67043328


def dot(a, b, dims):
    return lax.dot_general(a, b, (dims, ((), ())), preferred_element_type=F32)


NN, NT, TN = ((1,), (0,)), ((1,), (1,)), ((0,), (0,))


def normed(h):
    wide = h.astype(F32)
    scale = lax.rsqrt(jnp.mean(wide * wide, -1, keepdims=True) + 1e-6)
    return (wide * scale).astype(BF16)


def call(body, name, grid, in_specs, out_specs, out_shape, scratch, flops, moved, sends=None, limit=VMEM_LIMIT):
    remote = {} if sends is None else {"collective_id": sends, "has_side_effects": True}
    return pl.pallas_call(
        body,
        grid=grid,
        in_specs=in_specs,
        out_specs=out_specs,
        out_shape=out_shape,
        scratch_shapes=scratch,
        name=name,
        compiler_params=pltpu.CompilerParams(dimension_semantics=("arbitrary",) * len(grid), vmem_limit_bytes=limit, **remote),
        cost_estimate=pl.CostEstimate(flops=flops, bytes_accessed=moved, transcendentals=0),
    )


def once(shape, index):
    return pl.BlockSpec(shape, index, pipeline_mode=pl.Buffered(1))


def shape(dims, dtype):
    return jax.ShapeDtypeStruct(dims, dtype)


class Place:
    def __init__(self):
        s, r = lax.axis_index("s"), lax.axis_index("r")
        self.s, self.r = s, r
        self.x, self.c = s // 2, s % 2
        self.s_core, self.s_x = s + 1 - 2 * self.c, (s + 2) % 4
        self.s_both = (self.s_core + 2) % 4
        self.r_y, self.r_z = (r + 2) % 4, r + 1 - 2 * (r % 2)
        self.r_yz = (self.r_z + 2) % 4
        self.core, self.over_x = {"s": self.s_core}, {"s": self.s_x}
        self.over_y, self.over_z = {"r": self.r_y}, {"r": self.r_z}

    def meet(self):
        barrier = pltpu.get_barrier_semaphore()
        for one in (self.core, self.over_x, self.over_y, self.over_z):
            pl.semaphore_signal(barrier, inc=1, device_id=one, device_id_type=MESH)
        pl.semaphore_wait(barrier, 4)


def remote(src, dst, send, recv, device):
    return pltpu.make_async_remote_copy(
        src_ref=src, dst_ref=dst, send_sem=send, recv_sem=recv, device_id=device, device_id_type=MESH
    )


class Sum:
    FIRST = {"all": 0, "here": 0, "x": 0, "yz": 2}
    LAST = {"all": 4, "here": 4, "x": 2, "yz": 4}

    def __init__(self, place, kind, refs, outs, scratch):
        self.place, self.kind, self.refs, self.out = place, kind, refs, outs[0]
        self.square = outs[1] if kind != "x" else None
        self.local, self.send, self.recv = scratch[-3:]
        scratch = scratch[:-3]
        if kind != "yz":
            self.kept, self.got, self.far, self.got_x = scratch[:4]
            scratch = scratch[4:]
        if kind == "here":
            sent, self.got_1, self.got_2 = scratch
            self.near, self.pair = sent.at[0], sent.at[1]
            self.refs = [self.kept.at[0], self.kept.at[1], self.near, self.pair]
        elif kind != "x":
            self.near, self.got_1, self.pair, self.got_2 = scratch
        half = self.out.shape[0] // 2
        self.top, self.low = pl.ds(0, half), pl.ds(half, half)

    @staticmethod
    def scratch(kind, rows, cols):
        one = lambda *lead: pltpu.VMEM((*lead, rows, cols), BF16)
        to_x = [one(2), one(2), one(), one()] if kind != "yz" else []
        to_yz = [one(2), one(), one()] if kind == "here" else [one()] * 4 if kind != "x" else []
        return to_x + to_yz + [pltpu.SemaphoreType.DMA((k,)) for k in (2, 7, 7)]

    def copies(self, phase):
        p, over = self.place, lambda i, src, dst, to: remote(src, dst, self.send.at[i], self.recv.at[i], to)
        if phase == 0:
            return [over(i, self.refs[2 + i], self.got.at[i], p.core) for i in range(2)]
        if phase == 1:
            return [over(2, self.far, self.got_x, p.over_x)]
        if phase == 2:
            return [
                over(3, self.near.at[self.top], self.got_1.at[self.top], p.over_y),
                over(4, self.near.at[self.low], self.got_1.at[self.low], p.over_z),
            ]
        return [
            over(5, self.pair.at[self.top], self.got_2.at[self.top], p.over_z),
            over(6, self.pair.at[self.low], self.got_2.at[self.low], p.over_y),
        ]

    def locals(self):
        if self.kind == "here":
            return []
        if self.kind == "yz":
            return [pltpu.make_async_copy(self.refs[0], self.near, self.local.at[0])]
        return [pltpu.make_async_copy(self.refs[i], self.kept.at[i], self.local.at[i]) for i in range(2)]

    def run(self, phase):
        x = self.place.x
        wide = lambda ref: ref.astype(F32)
        if phase == 0:
            for one in self.locals() + self.copies(0):
                one.start()
            return
        if phase == 2 and self.kind == "yz":
            for one in self.locals():
                one.start()
                one.wait()
        else:
            for one in self.copies(phase - 1):
                one.wait()
        if phase == 1:
            for one in self.locals():
                one.wait()
            self.far[...] = (wide(self.kept[1 - x]) + wide(self.got[1 - x])).astype(BF16)
        elif phase == 2 and self.kind != "yz":
            into = self.out if self.kind == "x" else self.near
            into[...] = (wide(self.kept[x]) + wide(self.got[x]) + wide(self.got_x[...])).astype(BF16)
        elif phase == 3:
            self.pair[...] = (wide(self.near[...]) + wide(self.got_1[...])).astype(BF16)
        elif phase == 4:
            total = (wide(self.pair[...]) + wide(self.got_2[...])).astype(BF16)
            self.out[...] = total
            self.square[...] = jnp.full(self.square.shape, jnp.sum(wide(total) * wide(total)), F32)
        if phase < Sum.LAST[self.kind]:
            for one in self.copies(phase):
                one.start()


def timeline(sizes, kinds, steps, step_us, release=None):
    rate = {"core": 4e5, "x": 4.6e4, "y": 4.6e4, "z": 4.6e4}
    free = dict.fromkeys(rate, 0.0)
    parts = {0: (("core", 2.0),), 1: (("x", 1.0),), 2: (("y", 0.5), ("z", 0.5)), 3: (("y", 0.5), ("z", 0.5))}
    phase = [Sum.FIRST[kind] for kind in kinds]
    ready, order, now, k = list(release or [0.0] * len(sizes)), [], 0.0, 0
    while any(p <= Sum.LAST[kind] for p, kind in zip(phase, kinds)):
        waiting = [i for i, kind in enumerate(kinds) if phase[i] <= Sum.LAST[kind]]
        able = [i for i in waiting if ready[i] <= now]
        if not able and k < steps:
            k += 1
            now = max(now, k * step_us)
            continue
        i = min(able or waiting, key=lambda j: (ready[j], -phase[j], j))
        now = max(now, ready[i])
        order.append((k, i, phase[i]))
        ends = [now]
        for link, share in parts.get(phase[i], ()):
            free[link] = max(free[link], now) + share * sizes[i][0] * sizes[i][1] * 2 / rate[link]
            ends.append(free[link] + 2.0)
        ready[i] = max(ends)
        phase[i] += 1
    return order


class Load:
    def __init__(self, id, jobs):
        self.id = id
        self.kinds = [kind for kind, _, _ in jobs]
        self.parts = [part for _, _, part in jobs]
        self.sizes = [
            tuple(part[2] if part and part[0] == i else size for i, size in enumerate(terms[0].shape)) for _, terms, part in jobs
        ]
        self.counts = [len(terms) for _, terms, _ in jobs]
        self.args = [ref for _, terms, _ in jobs for ref in terms]
        self.in_specs = [pl.BlockSpec(memory_space=pl.ANY)] * len(self.args)
        here = lambda *_: (0, 0)
        results = [
            each for size, kind in zip(self.sizes, self.kinds) for each in [(size, BF16)] + ([] if kind == "x" else [((8, 128), F32)])
        ]
        self.out_specs = [once(size, here) for size, _ in results]
        self.out_shape = [shape(size, dtype) for size, dtype in results]
        self.scratch = [ref for size, kind in zip(self.sizes, self.kinds) for ref in Sum.scratch(kind, *size)]

    def sums(self, place, ins, outs, scratch):
        made = []
        for kind, part, size, count in zip(self.kinds, self.parts, self.sizes, self.counts):
            terms, ins = ins[:count], ins[count:]
            if part is not None:
                at = pl.ds(*part[1:])
                terms = [ref.at[at] if part[0] == 0 else ref.at[:, at] for ref in terms]
            n = 1 if kind == "x" else 2
            m = len(Sum.scratch(kind, *size))
            made.append(Sum(place, kind, terms, outs[:n], scratch[:m]))
            outs, scratch = outs[n:], scratch[m:]
        return made

    def results(self, outs):
        made = []
        for kind in self.kinds:
            n = 1 if kind == "x" else 2
            made.append(outs[0] if n == 1 else (outs[0], outs[1]))
            outs = outs[n:]
        return made


def carried(body, load, own_in, own_out, steps, step_us, hooks):
    order = timeline(load.sizes, load.kinds, steps * hooks, step_us / hooks)

    def both(*refs):
        n_in, n_out, n_scratch = len(load.in_specs), len(load.out_specs), len(load.scratch)
        ins, refs = refs[:own_in], refs[own_in:]
        more_in, refs = refs[:n_in], refs[n_in:]
        outs, refs = refs[:own_out], refs[own_out:]
        more_out, refs = refs[:n_out], refs[n_out:]
        scratch, more_scratch = refs[: len(refs) - n_scratch], refs[len(refs) - n_scratch :]
        place = Place()
        step = pl.program_id(0)
        sums = load.sums(place, more_in, more_out, more_scratch)

        def act(at):
            todo = [(i, phase) for when, i, phase in order if when == at]
            if todo:

                @pl.when(step == min(at // hooks, steps - 1))
                def _():
                    if at == 0:
                        place.meet()
                    for i, phase in todo:
                        sums[i].run(phase)

        def pause(now):
            for at in range(now, steps * hooks, hooks):
                act(at)

        pause(0)
        body(*ins, *outs, *scratch, **({"pause": pause} if hooks > 1 else {}))
        act(steps * hooks)

    return both


def call_with(load, step_us, hooks, body, name, grid, in_specs, out_specs, out_shape, scratch, flops, moved, args):
    if load is None:
        outs = call(body, name, grid, in_specs, out_specs, out_shape, scratch, flops, moved)(*args)
        return list(outs), []
    outs = call(
        carried(body, load, len(in_specs), len(out_specs), grid[0], step_us, hooks),
        name,
        grid,
        in_specs + load.in_specs,
        out_specs + load.out_specs,
        out_shape + load.out_shape,
        scratch + load.scratch,
        flops,
        moved,
        load.id,
    )(*args, *load.args)
    return list(outs[: len(out_specs)]), load.results(outs[len(out_specs) :])


def spread(acc, rows, refs):
    c = lax.axis_index("s") % 2
    for i, ref in enumerate(refs):
        at = (i % 2) * 2 + (c if i < 2 else 1 - c)
        ref[...] = acc[pl.ds(pl.multiple_of(at * rows, rows), rows), :].astype(BF16)


def spread_shapes(rows, cols, count=4):
    return [shape((rows, cols), BF16)] * count


def spread_specs(rows, cols, count=4):
    return [once((rows, cols), lambda *_: (0, 0))] * count


def clear(step, *refs):
    @pl.when(step == 0)
    def _():
        for ref in refs:
            ref[...] = jnp.zeros_like(ref)


class Fetch:
    COPIES = 9

    def __init__(self, place, own, full, columns, send, recv, local, stage=None):
        self.place, self.own, self.full, self.columns = place, own, full, columns
        self.send, self.recv, self.local, self.stage = send, recv, local, stage

    def part(self, block, quarter=None):
        rows = self.own.shape[0]
        if self.columns is None:
            if quarter is None:
                return self.full.at[pl.ds(pl.multiple_of(block * rows, rows), rows)]
            return self.full.at[pl.ds(pl.multiple_of(block * rows + quarter * (rows // 4), rows // 4), rows // 4)]
        start, width = self.columns
        across = pl.ds(start, width) if quarter is None else pl.ds(pl.multiple_of(start + quarter * (width // 4), 128), width // 4)
        return self.full.at[pl.ds(pl.multiple_of(block * rows, rows), rows), across]

    def mine(self, quarter=None):
        rows = self.own.shape[0]
        if self.columns is None:
            return self.own if quarter is None else self.own.at[pl.ds(pl.multiple_of(quarter * (rows // 4), rows // 4), rows // 4)]
        start, width = self.columns
        across = pl.ds(start, width) if quarter is None else pl.ds(pl.multiple_of(start + quarter * (width // 4), 128), width // 4)
        return self.own.at[:, across]

    def copy(self, i):
        p = self.place
        over = lambda src, dst, to: remote(src, dst, self.send.at[i], self.recv.at[i], to)
        if i == 0:
            return over(self.mine(), self.part(p.s), p.core)
        if i in (1, 2):
            q = p.r if i == 1 else p.r_yz
            return over(self.mine(q), self.part(p.s, q), p.over_x)
        if i in (3, 4):
            return over(self.part(p.s_x, p.r), self.part(p.s_x, p.r), p.over_y if i == 3 else p.over_z)
        q = (p.r, p.r_yz, p.r_y, p.r_z)[i - 5]
        return over(self.part(p.s_x, q), self.part(p.s_x, q), p.core)

    def received(self, i):
        p = self.place
        if i == 0:
            return self.part(p.s_core)
        block, q = [(p.s_x, p.r), (p.s_x, p.r_yz), (p.s_x, p.r_y), (p.s_x, p.r_z)][i - 1] if i < 5 else (p.s_both, (p.r, p.r_yz, p.r_y, p.r_z)[i - 5])
        return self.part(block, q)

    def start(self, *which):
        for i in which:
            self.copy(i).start()

    def arrived(self, i):
        here = self.received(i)
        remote(here, here, self.send.at[i], self.recv.at[i], self.place.core).wait_recv()

    def begin(self):
        self.start(1, 0)
        into = self.stage if self.stage is not None else self.part(self.place.s)
        pltpu.make_async_copy(self.mine(), into, self.local.at[0]).start()

    def begin_last(self):
        self.start(2)

    def relay(self):
        self.arrived(1)
        self.start(3, 4, 5)
        if self.stage is not None:
            pltpu.make_async_copy(self.mine(), self.stage, self.local.at[0]).wait()
            pltpu.make_async_copy(self.stage, self.part(self.place.s), self.local.at[1]).start()

    def hand_over(self):
        self.arrived(3)
        self.start(7)
        self.arrived(4)
        self.start(8)

    def hand_last(self):
        self.arrived(2)
        self.start(6)

    def finish(self):
        if self.stage is not None:
            pltpu.make_async_copy(self.stage, self.part(self.place.s), self.local.at[1]).wait()
        else:
            pltpu.make_async_copy(self.mine(), self.part(self.place.s), self.local.at[0]).wait()
        for i in (0, 5, 6, 7, 8):
            self.arrived(i)
        for i in range(self.COPIES):
            self.copy(i).wait_send()


RUN = 512


def project_body(h_ref, *refs):
    g, u, d, refs = *refs[:3], refs[3:]
    gate_ref, up_ref, prod_ref = refs[:3]
    full, refs = refs[3:5], refs[5:]
    a_all, wg, wu, stage_d0, stage_g1, send, recv, local = refs
    run, tile = pl.program_id(0), pl.program_id(1)
    step = run * pl.num_programs(1) + tile
    place = Place()
    ff = wg.shape[1]
    plan = [(own.at[0], whole, across, None) for across in ((0, 512), (512, 1024), (1536, 1024)) for own, whole in ((g, wg), (u, wu))]
    plan += [(d.at[0], full[0], None, stage_d0), (g.at[1], full[1], (0, ff), stage_g1)]
    fetches = [
        Fetch(place, mine, whole, columns, send.at[i], recv.at[i], local.at[i], stage) for i, (mine, whole, columns, stage) in enumerate(plan)
    ]

    def act(when, *moves):
        @pl.when(step == when)
        def _():
            for numbers, *what in moves:
                for each in what:
                    for number in numbers:
                        getattr(fetches[number], each)()

    @pl.when(step == 0)
    def _():
        place.meet()

    a, b, c, d0, g1 = (0, 1), (2, 3), (4, 5), (6,), (7,)
    act(0, (a, "begin", "begin_last"), (b, "begin", "begin_last"), (a, "relay", "hand_over", "hand_last", "finish"))
    act(1, (b, "relay"), (c, "begin", "begin_last"))
    act(4, (b, "hand_over", "hand_last", "finish"), (d0, "begin", "begin_last"))
    act(6, (c, "relay"))
    act(8, (g1, "begin", "begin_last"))
    act(9, (c, "hand_over", "hand_last"))
    act(11, (c, "finish"), (d0, "relay"))
    act(14, (d0, "hand_over", "hand_last"))
    act(16, (g1, "relay"))
    rows = h_ref.shape[0]
    mine = pl.ds(pl.multiple_of(tile * rows, rows), rows)

    @pl.when(run == 0)
    def _():
        a_all[mine, :] = normed(h_ref[...])

    a = a_all[mine, :]
    part = RUN // 2
    front = lambda i: [
        dot(a, w[:, pl.ds(pl.multiple_of(run * RUN + i * part, part), part)], NN) for w in (wg, wu)
    ]
    ahead = front(0)
    for i in range(2):
        gate, up = ahead
        if i == 0:
            ahead = front(1)
        at = slice(i * part, (i + 1) * part)
        gate_ref[:, at] = gate
        up_ref[:, at] = up
        prod_ref[:, at] = (gate * jax.nn.sigmoid(gate) * up).astype(BF16)
    act(19, (g1, "hand_over", "hand_last"), (d0, "finish"), (g1, "finish"))


def project(h, weights, tile=1024):
    n, d = h.shape
    ff = weights[0].shape[2]
    sizes = [one.shape[1:] for one in (weights[2], weights[0])]
    rows = pl.BlockSpec((tile, RUN), lambda i, j: (j, i))
    hbm = pl.BlockSpec(memory_space=pl.ANY)
    outs = call(
        project_body,
        "project",
        (ff // RUN, n // tile),
        [pl.BlockSpec((tile, d), lambda i, j: (jnp.where(i == 0, j, n // tile - 1), 0))] + [hbm] * 3,
        [rows] * 3 + [hbm] * 2,
        [shape((n, ff), F32), shape((n, ff), F32), shape((n, ff), BF16)]
        + [shape((high * 4, cols), BF16) for high, cols in sizes],
        [pltpu.VMEM((n, d), BF16), pltpu.VMEM((d, ff), BF16), pltpu.VMEM((d, ff), BF16)]
        + [pltpu.VMEM(size, BF16) for size in sizes]
        + [pltpu.SemaphoreType.DMA((8, 9)), pltpu.SemaphoreType.DMA((8, 9)), pltpu.SemaphoreType.DMA((8, 2))],
        4 * n * d * ff,
        n * ff * 10,
        0,
    )(h, *weights)
    return outs[:3], outs[3:]


def down_body(h_ref, prod_ref, wd_ref, u_ref, d_ref, out_ref, full_u, full_d, stage_u, stage_d, send, recv, local):
    step = pl.program_id(0)
    place = Place()
    plan = [(u_ref.at[1], full_u, (0, u_ref.shape[2]), stage_u), (d_ref.at[1], full_d, None, stage_d)]
    fetches = [
        Fetch(place, mine, whole, columns, send.at[i], recv.at[i], local.at[i], stage) for i, (mine, whole, columns, stage) in enumerate(plan)
    ]

    def act(when, *moves):
        @pl.when(step == when)
        def _():
            if when == 0:
                place.meet()
            for numbers, *what in moves:
                for each in what:
                    for number in numbers:
                        getattr(fetches[number], each)()

    act(0, ((0, 1), "begin", "begin_last"))
    act(3, ((0,), "relay"))
    act(5, ((1,), "relay"))
    act(6, ((0,), "hand_over"))
    out_ref[...] = h_ref[...] + dot(prod_ref[...], wd_ref[...], NN).astype(BF16)
    act(pl.num_programs(0) - 1, ((0,), "hand_last"), ((1,), "hand_over", "hand_last"), ((0, 1), "finish"))


def down(h, prod, wd, w_up, w_down, tile=512):
    n, d = h.shape
    ff = wd.shape[0]
    rows = lambda width: pl.BlockSpec((tile, width), lambda i: (i, 0))
    hbm = pl.BlockSpec(memory_space=pl.ANY)
    return call(
        down_body,
        "down",
        (n // tile,),
        [rows(d), rows(ff), once((ff, d), lambda i: (0, 0)), hbm, hbm],
        [rows(d), hbm, hbm],
        [shape((n, d), BF16), shape((d, ff), BF16), shape((ff, d), BF16)],
        [pltpu.VMEM(one.shape[1:], BF16) for one in (w_up, w_down)]
        + [pltpu.SemaphoreType.DMA((2, 9)), pltpu.SemaphoreType.DMA((2, 9)), pltpu.SemaphoreType.DMA((2, 2))],
        2 * n * d * ff,
        n * ff * 2,
        7,
    )(h, prod, wd, w_up, w_down)


def slopes(gate, up, dprod):
    s = jax.nn.sigmoid(gate)
    silu = gate * s
    return silu, (dprod * silu).astype(BF16), (dprod * up * (s + silu * (1 - s))).astype(BF16)


def last_body(part, h_ref, dy_ref, wg_ref, wu_ref, wd_ref, dgate_ref, dup_ref, *rest):
    outs, (acc_g, acc_u, acc_d) = rest[:10], rest[10:]
    step = pl.program_id(0)
    clear(step, acc_g, acc_u, acc_d)
    a = normed(h_ref[...])
    dy = dy_ref[...]
    a_t, dy_t = a.T, dy.T
    parts = [slice(i, i + part) for i in range(0, wg_ref.shape[1], part)]
    front = lambda at: (dot(a, wg_ref[:, at], NN), dot(a, wu_ref[:, at], NN), dot(dy, wd_ref[at, :], NT))
    ahead = front(parts[0])
    for i, at in enumerate(parts):
        gate, up, dprod = ahead
        if i + 1 < len(parts):
            ahead = front(parts[i + 1])
        silu, dup, dgate = slopes(gate, up, dprod.astype(BF16).astype(F32))
        dgate_ref[:, at] = dgate
        dup_ref[:, at] = dup
        acc_g[:, at] += dot(a_t, dgate, NN)
        acc_u[:, at] += dot(a_t, dup, NN)
        acc_d[:, at] += dot(dy_t, (silu * up).astype(BF16), NN)

    @pl.when(step == pl.num_programs(0) - 1)
    def _():
        rows = acc_g.shape[0] // 4
        spread(acc_g, rows, outs[:4])
        spread(acc_u, rows, outs[4:8])
        c = lax.axis_index("s") % 2
        rows = acc_d.shape[1] // 2
        for core, ref in ((c, outs[8]), (1 - c, outs[9])):
            ref[...] = acc_d[:, pl.ds(pl.multiple_of(core * rows, rows), rows)].T.astype(BF16)


def last(h, dy, wg, wu, wd, run, runs, load=None, step_us=1.0, tile=512, part=256):
    n, d = h.shape
    ff = wg.shape[1] // runs
    rows = lambda width: pl.BlockSpec((tile, width), lambda i: (i, 0))
    columns = lambda: once((d, ff), lambda i: (0, run))
    outs, done = call_with(
        load,
        step_us,
        1,
        functools.partial(last_body, part),
        f"last{run}",
        (n // tile,),
        [rows(d), rows(d), columns(), columns(), once((ff, d), lambda i: (run, 0))],
        [rows(ff), rows(ff)] + spread_specs(d // 4, ff, 8) + spread_specs(ff // 2, d, 2),
        [shape((n, ff), BF16)] * 2 + spread_shapes(d // 4, ff, 8) + spread_shapes(ff // 2, d, 2),
        [pltpu.VMEM((d, ff), F32)] * 3,
        12 * n * d * ff,
        n * ff * 4,
        (h, dy, wg, wu, wd),
    )
    return outs[0], outs[1], outs[2:6], outs[6:10], outs[10:12], done


def inward_body(runs, h_ref, by_ref, *rest, pause):
    dgates, dups, (wg_ref, wu_ref, out_ref) = rest[:runs], rest[runs : 2 * runs], rest[2 * runs :]
    ff = dgates[0].shape[1]
    total = lambda parts, w: sum(dot(p[...], w[:, i * ff : (i + 1) * ff], NT) for i, p in enumerate(parts)).astype(BF16)
    da = total(dgates, wg_ref)
    pause(1)
    da = (da + total(dups, wu_ref)).astype(F32)
    wide = h_ref[...].astype(F32)
    scale = lax.rsqrt(jnp.mean(wide * wide, -1, keepdims=True) + 1e-6)
    along = jnp.mean(da * wide, -1, keepdims=True)
    dh = da * scale - wide * (scale * scale * scale * along)
    out_ref[...] = by_ref[...] + dh.astype(BF16)


def inward(h, by, dgates, dups, wg, wu, load=None, step_us=1.0, tile=512):
    n, d = h.shape
    ff = wg.shape[1]
    runs = len(dgates)
    rows = lambda width: pl.BlockSpec((tile, width), lambda i: (i, 0))
    outs, done = call_with(
        load,
        step_us,
        2,
        functools.partial(inward_body, runs),
        "inward",
        (n // tile,),
        [rows(d), rows(d)] + [rows(ff // runs)] * (2 * runs) + [once((d, ff), lambda i: (0, 0))] * 2,
        [rows(d)],
        [shape((n, d), BF16)],
        [],
        4 * n * d * ff,
        n * ff * 4,
        (h, by, *dgates, *dups, wg, wu),
    )
    return outs[0], done


def outer_body(by_ref, prod_ref, *rest):
    outs, acc = rest[:4], rest[4]
    step = pl.program_id(0)
    clear(step, acc)
    acc[...] += dot(by_ref[...].T, prod_ref[...], NN)

    @pl.when(step == pl.num_programs(0) - 1)
    def _():
        c = lax.axis_index("s") % 2
        rows = acc.shape[1] // 4
        for i, ref in enumerate(outs):
            block = (i % 2) * 2 + (c if i < 2 else 1 - c)
            ref[...] = acc[:, pl.ds(pl.multiple_of(block * rows, rows), rows)].T.astype(BF16)


def outer(by, prod, load=None, step_us=1.0, tile=512):
    n, d = by.shape
    ff = prod.shape[1]
    rows = lambda width: pl.BlockSpec((tile, width), lambda i: (i, 0))
    return call_with(
        load,
        step_us,
        1,
        outer_body,
        "outer",
        (n // tile,),
        [rows(d), rows(ff)],
        spread_specs(ff // 4, d),
        spread_shapes(ff // 4, d),
        [pltpu.VMEM((d, ff), F32)],
        2 * n * d * ff,
        n * ff * 2,
        (by, prod),
    )


def first_body(part, count, squares, load, runs, tiles, step_us, h_ref, by_ref, gate_ref, up_ref, wd_ref, *refs):
    n_in, n_out, n_scratch = len(load.in_specs), len(load.out_specs), len(load.scratch)
    others, refs = refs[:squares], refs[squares:]
    ins, refs = refs[:n_in], refs[n_in:]
    outs, refs = refs[:n_out], refs[n_out:]
    own_outs, factor_ref, refs = refs[: 4 * runs], refs[4 * runs], refs[4 * runs + 1 :]
    (acc_g, acc_u, mine, got_core, both, got_x, send, recv), refs = refs[:8], refs[8:]
    scratch, refs = refs[:n_scratch], refs[n_scratch:]
    run, tile = pl.program_id(0), pl.program_id(1)
    step = run * tiles + tile
    place = Place()
    size = (acc_g.shape[0] // 4, acc_g.shape[1])
    per = len(Sum.scratch("here", *size))
    own = [Sum(place, "here", None, own_outs[2 * i : 2 * i + 2], refs[per * i : per * i + per]) for i in range(2 * runs)]
    sums = load.sums(place, ins, outs, scratch) + own
    release = [0.0] * len(load.sizes) + [(i // 2 + 1) * tiles * step_us for i in range(2 * runs)]
    order = timeline(load.sizes + [size] * len(own), load.kinds + ["here"] * len(own), runs * tiles, step_us, release)

    def act(at):
        todo = [(i, phase) for when, i, phase in order if when == at]
        if todo:

            @pl.when(step == min(at, runs * tiles - 1))
            def _():
                if at == 0:
                    place.meet()
                for i, phase in todo:
                    sums[i].run(phase)

    for at in range(runs * tiles):
        act(at)
    clear(tile, acc_g, acc_u)
    a_t = normed(h_ref[...]).T
    by = by_ref[...]
    parts = [slice(i, i + part) for i in range(0, wd_ref.shape[0], part)]
    front = lambda at: dot(by, wd_ref[at, :], NT)
    ahead = front(parts[0])
    for i, at in enumerate(parts):
        dprod = ahead.astype(BF16).astype(F32)
        if i + 1 < len(parts):
            ahead = front(parts[i + 1])
        _, dup, dgate = slopes(gate_ref[:, at], up_ref[:, at], dprod)
        acc_g[:, at] += dot(a_t, dgate, NN)
        acc_u[:, at] += dot(a_t, dup, NN)

    for number in range(runs):

        @pl.when(step == number * tiles + tiles - 1)
        def _(number=number):
            spread(acc_g, size[0], own[2 * number].refs)
            spread(acc_u, size[0], own[2 * number + 1].refs)

    act(runs * tiles)

    @pl.when(step == runs * tiles - 1)
    def _():
        total = sum(ref[...] for ref in others) + sum(one.square[...] for one in sums)
        mine[...] = total
        hop = remote(mine, got_core, send.at[0], recv.at[0], place.core)
        hop.start()
        hop.wait()
        both[...] = mine[...] + got_core[...]
        hop = remote(both, got_x, send.at[1], recv.at[1], place.over_x)
        hop.start()
        hop.wait()
        factor_ref[...] = jnp.minimum(1.0, 0.5 * lax.rsqrt((both[...] + got_x[...]) / count + 1e-30))


def first(h, by, gate, up, wd, load, squares, count, step_us, tile=512, part=256):
    n, d = h.shape
    runs, tiles = gate.shape[1] // RUN, n // tile
    rows = pl.BlockSpec((tile, d), lambda i, j: (j, 0))
    kept = pl.BlockSpec((tile, RUN), lambda i, j: (j, i))
    whole = once((8, 128), lambda *_: (0, 0))
    size = (d // 4, RUN)
    outs = call(
        functools.partial(first_body, part, count, len(squares), load, runs, tiles, step_us),
        "first",
        (runs, tiles),
        [rows, rows, kept, kept, pl.BlockSpec((RUN, d), lambda i, j: (i, 0))] + [whole] * len(squares) + load.in_specs,
        load.out_specs + [once(size, lambda *_: (0, 0)), whole] * (2 * runs) + [whole],
        load.out_shape + [shape(size, BF16), shape((8, 128), F32)] * (2 * runs) + [shape((8, 128), F32)],
        [pltpu.VMEM((d, RUN), F32)] * 2
        + [pltpu.VMEM((8, 128), F32)] * 4
        + [pltpu.SemaphoreType.DMA((2,))] * 2
        + load.scratch
        + Sum.scratch("here", *size) * (2 * runs),
        6 * n * d * gate.shape[1],
        n * gate.shape[1] * 8,
        load.id,
        limit=WHOLE,
    )(h, by, gate, up, wd, *squares, *load.args)
    n_out = len(load.out_specs)
    own = outs[n_out:-1:2]
    return own[0::2], own[1::2], load.results(outs[:n_out]), outs[-1]


def adamw(w, m, v, g):
    m = 0.9 * m + 0.1 * g
    v = 0.95 * v + 0.05 * g * g
    step = m * lax.rsqrt(v + 1e-8) + 0.1 * w
    return (w - 0.02 * step).astype(BF16), m, v


def update_body(edges, factor_ref, *refs):
    total = sum(len(edge) - 1 for per_layer in edges for edge in per_layer)
    grads, refs = refs[:total], refs[total:]
    states, news = refs[:9], refs[9:]
    turn = pl.program_id(0)
    factor = factor_ref[0, 0]
    k = 0
    for i, per_layer in enumerate(edges):
        for number, edge in enumerate(per_layer):
            for low, high in zip(edge, edge[1:]):

                @pl.when((turn >= low) & (turn < high))
                def _(ref=grads[k], i=i, number=number):
                    w, m, v = (states[3 * which + i][number] for which in range(3))
                    for which, one in enumerate(adamw(w.astype(F32), m, v, ref[...].astype(F32) * factor)):
                        news[3 * which + i][number] = one

                k += 1


def update(factor, pieces, states, turns=10):
    specs, edges, args = [pl.BlockSpec(memory_space=pltpu.SMEM)], [], [factor]
    state_specs = []
    for i, per_layer in enumerate(pieces):
        layers, rows, cols = states[i].shape
        tall = i == 2
        block = (rows // turns, cols) if tall else (rows, cols // turns)
        edges.append([])
        for parts in per_layer:
            edge = [0]
            for part in parts:
                low = edge[-1]
                edge.append(low + (part.shape[0] // block[0] if tall else part.shape[1] // block[1]))

                def index(turn, low=low, top=edge[-1] - low - 1, tall=tall):
                    at = jnp.clip(turn - low, 0, top)
                    return (at, 0) if tall else (0, at)

                specs.append(pl.BlockSpec(block, index))
                args.append(part)
            edges[-1].append(edge)
        state_specs.append(pl.BlockSpec((layers, *block), (lambda turn: (0, turn, 0)) if tall else (lambda turn: (0, 0, turn))))
    return call(
        functools.partial(update_body, edges),
        "update",
        (turns,),
        specs + state_specs * 3,
        state_specs * 3,
        [shape(one.shape, one.dtype) for one in states],
        [],
        1000000,
        1000000,
        limit=SMALL,
    )(*args, *states)


def solution(mesh):
    ns = mesh.shape["s"]

    def step(x, dy, *arrays):
        weights, m, v = (arrays[i : i + 3] for i in (0, 3, 6))
        h0, dy = x[0], dy[0]
        (gate, up, prod), (wd0, wg1) = project(h0, weights)
        h1, wu1, wd1 = down(h0, prod, wd0, weights[1], weights[2])
        a = last(h1, dy, wg1, wu1, wd1, 0, 2)
        b = last(h1, dy, wg1, wu1, wd1, 1, 2, Load(1, [("all", a[2], None), ("all", a[3], None)]), 9.0)
        g1a, u1a = b[5]
        d1 = [a[4][0], b[4][0], a[4][1], b[4][1]]
        high, low = (0, 0, 384), (0, 384, 256)
        load = Load(2, [("all", b[2], None), ("all", b[3], None), ("x", d1, high)])
        by, (g1b, u1b, d1a) = inward(h1, dy, [a[0], b[0]], [a[1], b[1]], wg1, wu1, load, 6.2)
        d0, (d1a, d1b) = outer(by, prod, Load(3, [("yz", [d1a], None), ("x", d1, low)]), 3.1)
        load = Load(4, [("all", d0, high), ("all", d0, low), ("yz", [d1b], None)])
        squares = [one[1] for one in (g1a, u1a, g1b, u1b, d1a)]
        g0, u0, (d0a, d0b, d1b), factor = first(h0, by, gate, up, wd0, load, squares, ns * sum(w.size for w in weights), 1.8)
        parts = lambda *ones: [one[0] for one in ones]
        pieces = [
            [g0, parts(g1a, g1b)],
            [u0, parts(u1a, u1b)],
            [parts(d0a, d0b), parts(d1a, d1b)],
        ]
        return tuple(update(factor, pieces, [*weights, *m, *v]))

    states, cut = P(("rep", "r", "s"), None, None), P(None, "s", None)
    return jax.shard_map(
        step,
        mesh=mesh,
        in_specs=(states, states) + (cut,) * 9,
        out_specs=(P("rep", "s", None),) * 9,
        check_vma=False,
    )
```
